32 devices in a mesh: shard: 8 (over z, x), grp: 4 (over y, core).
Axes of the slice: x: 2, y: 2, z: 4, core: 2. Of those that a mesh axis runs over, the one named last changes fastest.
Arguments:
- table_t: bfloat16 [100, 622592], P(None, ('shard', 'grp')), may hold values from -6 to 6
- req_rows: int32 [1024, 128], P(('shard', 'grp')), may hold values from 0 to 19455
- count1: int32 [1024], P(('shard', 'grp')), may hold values from 1 to 128, as said below
- frontier_list: int32 [11, 32768], P(None, ('shard', 'grp')), may hold values from 0 to 4095, as said below
- req2_rows: int32 [1024, 128], P(('shard', 'grp')), may hold values from 0 to 1023
- count2: int32 [1024], P(('shard', 'grp')), may hold values from 1 to 128, as said below
- seed_list: int32 [16, 8192], P(None, ('shard', 'grp')), may hold values from 0 to 4095, as said below
- w1_self: bfloat16 [256, 100], replicated, may hold values from -0.625 to 0.625
- w1_neigh: bfloat16 [256, 100], replicated, may hold values from -1.25 to 1.25
- bias1: float32 [256], replicated, may hold values from -3 to 3
- w2_self: bfloat16 [47, 256], replicated, may hold values from -0.375 to 0.375
- w2_neigh: bfloat16 [47, 256], replicated, may hold values from -0.75 to 0.75
- bias2: float32 [47], replicated, may hold values from -3 to 3
Outputs:
- logits: float32 [47, 8192], P(None, ('shard', 'grp'))
The draws below stay inside these ranges and needn't reach their ends.
Inputs may be any that keep to these rules, and one draw needn't show every extreme that they name: count1[r * 32 + o] counts the live slots of the block that device r asks of device o; in every draw some devices are asked for 128 rows by every device. `frontier_list`: every entry o * 128 + j names a live slot (j below count1 of that block) of the asking device. count2[r * 32 + o] counts the live slots of the block that device r asks of device o; in every draw some devices are asked for 128 rows by every device. `seed_list`: every entry o * 128 + j names a live slot (j below count2 of that block) of the asking device.
All inputs are finite; a program needn't handle non-finite values.
Results may differ from the reference program's by a relative error of at most 0.0029.
Values may be sent and summed in bfloat16 or wider, within the bound.
No kernel may reach another device: no remote copies, remote signals or barrier semaphores. Data moves between devices by JAX's collectives and lax.ppermute only.
A program may use at most 64 MiB of HBM per device.

```python
import jax
import jax.numpy as jnp
from jax import lax

F = 100
H = 256
C = 47
K1 = 15
K2 = 10
ROWS_DEV = 19456
FRONT_DEV = 1024
SEED_DEV = 256
CAP = 128
CAP2 = 128
NODES = 622592
PAIRS = 1024
N_SHARD = 8
N_GRP = 4
DEVICES = 32


def counts_table(key, capacity):
    first_key, second_key = jax.random.split(key)
    base = jax.random.randint(first_key, (DEVICES, DEVICES), max(1, capacity // 8), capacity // 2 + 1)
    hottest = jax.random.permutation(second_key, DEVICES)[:max(1, DEVICES // 16)]
    is_hot = jnp.any(jnp.arange(DEVICES)[:, None] == hottest[None, :], axis=1)
    return jnp.where(is_hot[None, :], capacity, base).astype(jnp.int32)


def slot_table(key, counts, capacity, entries, per_device):
    first_key, second_key = jax.random.split(key)
    owners = jax.random.randint(first_key, (entries, DEVICES * per_device), 0, DEVICES)
    askers = jnp.broadcast_to((jnp.arange(DEVICES * per_device) // per_device)[None, :], owners.shape)
    live_count = counts[askers, owners]
    offset = jax.random.randint(second_key, owners.shape, 0, 1 << 30) % live_count
    return (owners * capacity + offset).astype(jnp.int32)


def draw_count1(key, part):
    return counts_table(jax.random.fold_in(key, 101), CAP).reshape(-1)


def draw_frontier_list(key, part):
    counts = counts_table(jax.random.fold_in(key, 101), CAP)
    return slot_table(jax.random.fold_in(key, 102), counts, CAP, K2 + 1, FRONT_DEV)


def draw_count2(key, part):
    return counts_table(jax.random.fold_in(key, 201), CAP2).reshape(-1)


def draw_seed_list(key, part):
    counts = counts_table(jax.random.fold_in(key, 201), CAP2)
    return slot_table(jax.random.fold_in(key, 202), counts, CAP2, K1 + 1, SEED_DEV)


def with_ends(values, rng, smallest, top_value):
    shape = values.shape
    index_at = [jax.random.randint(jax.random.fold_in(rng, axis), (), 0, shape[axis]) for axis in range(len(shape))]
    values = values.at[tuple(index_at)].set(smallest)
    longest = shape.index(max(shape))
    index_at[longest] = (index_at[longest] + 1) % shape[longest]
    return values.at[tuple(index_at)].set(top_value)


def block_levels(stream_key, shape, cuts, smallest, largest):
    level, own = 1.0, jax.random.fold_in(stream_key, 6)
    for axis_at, parts in cuts:
        steps = jnp.exp(jax.random.uniform(jax.random.fold_in(own, axis_at), (parts,), jnp.float32, smallest / len(cuts), largest / len(cuts)))
        level = level * jnp.repeat(steps, shape[axis_at] // parts).reshape([-1 if axis == axis_at else 1 for axis in range(len(shape))])
    return level


def gaussian(key, extent, width, most, cuts=(), kind=jnp.bfloat16):
    values = jax.random.normal(key, extent, jnp.float32) * width
    if len(cuts) > 0:
        values = block_levels(key, extent, cuts, -0.22, 0.18) * values
    return jnp.clip(values, min=-most, max=most).astype(kind)


def setup_inputs(seed: int = 0) -> dict:
    streams_of = jax.random.split(jax.random.key(seed), 14)
    table_t = gaussian(streams_of[0], (F, NODES), 1.0, 6.0, ((1, 32),))
    req_rows = with_ends(jax.random.randint(streams_of[1], (PAIRS, CAP), 0, ROWS_DEV), jax.random.fold_in(streams_of[1], 1), 0, ROWS_DEV - 1).astype(jnp.int32)
    count1 = draw_count1(jax.random.fold_in(streams_of[13], 71), 0)
    frontier_list = draw_frontier_list(jax.random.fold_in(streams_of[13], 71), 0)
    req2_rows = with_ends(jax.random.randint(streams_of[4], (PAIRS, CAP2), 0, FRONT_DEV), jax.random.fold_in(streams_of[4], 1), 0, FRONT_DEV - 1).astype(jnp.int32)
    count2 = draw_count2(jax.random.fold_in(streams_of[13], 71), 0)
    seed_list = draw_seed_list(jax.random.fold_in(streams_of[13], 71), 0)
    w1_self = gaussian(streams_of[7], (H, F), F ** -0.5, 0.625)
    w1_neigh = gaussian(streams_of[8], (H, F), (F // 4) ** -0.5, 1.25)
    bias1 = gaussian(streams_of[9], (H,), 0.5, 3.0, (), jnp.float32)
    w2_self = gaussian(streams_of[10], (C, H), H ** -0.5, 0.375)
    w2_neigh = gaussian(streams_of[11], (C, H), (H // 4) ** -0.5, 0.75)
    bias2 = gaussian(streams_of[12], (C,), 0.5, 3.0, (), jnp.float32)
    return dict(table_t=table_t, req_rows=req_rows, count1=count1, frontier_list=frontier_list, req2_rows=req2_rows, count2=count2, seed_list=seed_list, w1_self=w1_self, w1_neigh=w1_neigh, bias1=bias1, w2_self=w2_self, w2_neigh=w2_neigh, bias2=bias2)


def reference(table_t, req_rows, count1, frontier_list, req2_rows, count2, seed_list, w1_self, w1_neigh, bias1, w2_self, w2_neigh, bias2):
    devices = N_SHARD * N_GRP
    table_base = (jnp.arange(devices, dtype=jnp.int32) * ROWS_DEV)[:, None]
    front_base = (jnp.arange(devices, dtype=jnp.int32) * FRONT_DEV)[:, None]
    asked_one = req_rows.reshape(devices, devices, CAP)
    counts_one = count1.reshape(devices, devices)
    lists_one = frontier_list.reshape(K2 + 1, devices, FRONT_DEV).transpose(1, 0, 2)

    def layer_one(args):
        wanted, counts, picks = args
        columns = jnp.take(table_t, (wanted + table_base).reshape(-1).astype(jnp.int32), axis=1)
        is_live = (jnp.arange(CAP, dtype=jnp.int32)[None, :] < counts[:, None]).reshape(-1)
        columns = jnp.where(is_live[None, :], columns, jnp.zeros((), columns.dtype))
        picked = jnp.take(columns, picks.reshape(-1), axis=1).reshape(F, K2 + 1, FRONT_DEV)
        summed = (jnp.sum(picked[:, 1:].astype(jnp.float32), axis=1) / K2).astype(jnp.bfloat16)
        preact = jnp.dot(w1_self, picked[:, 0], preferred_element_type=jnp.float32)
        preact = preact + jnp.dot(w1_neigh, summed, preferred_element_type=jnp.float32) + bias1[:, None]
        return jax.nn.relu(preact).astype(jnp.bfloat16)

    hidden = lax.map(layer_one, (asked_one, counts_one, lists_one))
    hidden = hidden.transpose(1, 0, 2).reshape(H, devices * FRONT_DEV)
    asked_two = req2_rows.reshape(devices, devices, CAP2)
    counts_two = count2.reshape(devices, devices)
    lists_two = seed_list.reshape(K1 + 1, devices, SEED_DEV).transpose(1, 0, 2)

    def layer_two(args):
        wanted, counts, picks = args
        columns = jnp.take(hidden, (wanted + front_base).reshape(-1).astype(jnp.int32), axis=1)
        is_live = (jnp.arange(CAP2, dtype=jnp.int32)[None, :] < counts[:, None]).reshape(-1)
        columns = jnp.where(is_live[None, :], columns, jnp.zeros((), columns.dtype))
        picked = jnp.take(columns, picks.reshape(-1), axis=1).reshape(H, K1 + 1, SEED_DEV)
        near = jnp.sum(picked[:, 1:].astype(jnp.float32), axis=1) / K1
        result = jnp.dot(w2_self, picked[:, 0], preferred_element_type=jnp.float32)
        result = result + jnp.dot(w2_neigh.astype(jnp.float32), near, precision=lax.Precision.HIGHEST, preferred_element_type=jnp.float32)
        return result + bias2[:, None]

    logits = lax.map(layer_two, (asked_two, counts_two, lists_two))
    return logits.transpose(1, 0, 2).reshape(C, devices * SEED_DEV)
```

```python
import functools

import jax
import jax.numpy as jnp
from jax import lax
from jax.experimental import pallas as pl
from jax.experimental.pallas import tpu as pltpu
from jax.sharding import PartitionSpec as P

AXES = ("shard", "grp")
F32 = jnp.float32
BF16 = jnp.bfloat16
I32 = jnp.int32
WHOLE_VMEM = pl.BlockSpec(memory_space=pltpu.VMEM)
WHOLE_SMEM = pl.BlockSpec(memory_space=pltpu.SMEM)
IN_HBM = pl.BlockSpec(memory_space=pltpu.HBM)


def exchange(blocks):
    return lax.all_to_all(blocks, AXES, split_axis=0, concat_axis=0, tiled=True)


def params(mib):
    return pltpu.CompilerParams(vmem_limit_bytes=mib << 20)


def identity(n, dtype):
    rows = lax.broadcasted_iota(I32, (n, n), 0)
    lanes = lax.broadcasted_iota(I32, (n, n), 1)
    return jnp.where(rows == lanes, 1.0, 0.0).astype(dtype)


def fetch_kernel(word_ref, asked_ref, pairs_hbm, out_ref, pairs, buf, sem):
    blocks, feats, cap = out_ref.shape
    load = pltpu.make_async_copy(pairs_hbm, pairs, sem)
    load.start()
    load.wait()

    def gather(r, _):
        for j in range(cap):
            buf[r * cap + j] = pairs[word_ref[r, j] >> 17]
        return 0

    lax.fori_loop(0, blocks, gather, 0)
    eye = identity(feats, BF16)
    place = lax.broadcasted_iota(I32, (2 * cap, cap), 0).astype(F32).astype(BF16)
    twice = 2 * lax.broadcasted_iota(I32, (1, cap), 1)

    def turn(i, _):
        for u in range(4):
            r = i * 4 + u
            x = buf[pl.ds(pl.multiple_of(r * cap, cap), cap)].reshape(2 * cap, feats)
            y = lax.dot_general(eye, x, (((1,), (1,)), ((), ())), preferred_element_type=F32).astype(BF16)
            want = twice + ((asked_ref[pl.ds(r, 1), :] >> 16) & 1)
            want = jnp.broadcast_to(want.astype(F32), (2 * cap, cap)).astype(BF16)
            pick = jnp.where(want == place, jnp.ones((), BF16), jnp.zeros((), BF16))
            out_ref[r] = jnp.dot(y, pick, preferred_element_type=F32).astype(BF16)
        return 0

    lax.fori_loop(0, blocks // 4, turn, 0)


def fetch(asked, table_t):
    feats, n = table_t.shape
    blocks, cap = asked.shape
    pairs = table_t.T.reshape(n // 2, 2, feats)
    return pl.pallas_call(
        fetch_kernel,
        out_shape=jax.ShapeDtypeStruct((blocks, feats, cap), BF16),
        in_specs=[WHOLE_SMEM, WHOLE_VMEM, IN_HBM],
        out_specs=WHOLE_VMEM,
        scratch_shapes=[
            pltpu.VMEM((n // 2, 2, feats), BF16),
            pltpu.VMEM((blocks * cap, 2, feats), BF16),
            pltpu.SemaphoreType.DMA,
        ],
        compiler_params=params(20),
        name="fetch",
    )(asked, asked, pairs)


def own_weight(fanout):
    return 1 << fanout.bit_length()


def codes_kernel(own, count_ref, list_ref, out_ref):
    depth, nodes = list_ref.shape
    cap = out_ref.shape[0]
    o = pl.program_id(0)
    width = min(nodes, 256)
    zero = jnp.zeros((16, width), BF16)
    hit = [jnp.full((16, width), own if k == 0 else 1, BF16) for k in range(2)]

    def step(t, _):
        at = pl.multiple_of(t * width, width)
        local = list_ref[:, pl.ds(at, width)] - o * cap
        live = (local >= 0) & (local < count_ref[o])
        local = jnp.where(live, local, -1).astype(F32)
        want = [jnp.broadcast_to(local[k : k + 1], (16, width)).astype(BF16) for k in range(depth)]
        for g in range(cap // 16):
            slot = (lax.broadcasted_iota(I32, (16, width), 0) + g * 16).astype(F32).astype(BF16)
            total = jnp.where(want[0] == slot, hit[0], zero)
            for k in range(1, depth):
                total = total + jnp.where(want[k] == slot, hit[1], zero)
            out_ref[pl.ds(g * 16, 16), pl.ds(at, width)] = total
        return 0

    lax.fori_loop(0, nodes // width, step, 0)


def codes(counts, lists, cap, place):
    depth, nodes = lists.shape
    blocks = counts.shape[0]
    return pl.pallas_call(
        functools.partial(codes_kernel, own_weight(depth - 1)),
        grid=(blocks,),
        out_shape=place((blocks * cap, nodes), BF16),
        in_specs=[WHOLE_SMEM, WHOLE_VMEM],
        out_specs=pl.BlockSpec((cap, nodes), lambda o: (o, 0)),
        compiler_params=params(8),
        name="codes",
    )(counts, lists)


def choose_kernel(group, word_ref, out_ref):
    cap = word_ref.shape[1]
    nodes = out_ref.shape[0]
    one, zero = jnp.ones((16, cap), BF16), jnp.zeros((16, cap), BF16)
    per = out_ref.shape[1] // cap
    for u in range(per):
        asked = word_ref[pl.ds(pl.program_id(0) * per + u, 1), :] & 0xFFFF
        for base in range(0, nodes, group):
            local = asked - base
            local = jnp.where((local >= 0) & (local < group), local, -1).astype(F32)
            want = jnp.broadcast_to(local, (16, cap)).astype(BF16)
            for g in range(0, group, 16):
                node = (lax.broadcasted_iota(I32, (16, cap), 0) + g).astype(F32).astype(BF16)
                out_ref[pl.ds(base + g, 16), u * cap : (u + 1) * cap] = jnp.where(want == node, one, zero)


def choose(asked, nodes):
    blocks, cap = asked.shape
    per = 4
    return pl.pallas_call(
        functools.partial(choose_kernel, 256),
        grid=(blocks // per,),
        out_shape=pltpu.HBM((nodes, blocks * cap), BF16),
        in_specs=[WHOLE_VMEM],
        out_specs=pl.BlockSpec((nodes, per * cap), lambda r: (0, r)),
        compiler_params=params(8),
        name="choose",
    )(asked)


def wide(ref, first, last, lo, hi):
    return jnp.concatenate([ref[o, lo:hi] for o in range(first, last)], axis=1)


def split_codes(code, own):
    return jnp.where(code >= own, jnp.ones((), BF16), jnp.zeros((), BF16))


def layer_kernel(
    fanout, parts, got_ref, codes_hbm, choose_hbm, ws_ref, wn_ref, b_ref, w2_ref, out_ref, codes_v, choose_v, sems
):
    blocks, feats, cap = got_ref.shape
    own_w = own_weight(fanout)
    each = blocks // parts
    span = each * cap
    nodes = codes_v.shape[1]
    loads = [
        pltpu.make_async_copy(codes_hbm.at[pl.ds(i * span, span)], codes_v.at[pl.ds(i * span, span)], sems.at[i])
        for i in range(parts)
    ]
    cap2 = out_ref.shape[2]
    span2 = each * cap2
    loads2 = [
        pltpu.make_async_copy(
            choose_hbm.at[:, pl.ds(i * span2, span2)], choose_v.at[:, pl.ds(i * span2, span2)], sems.at[parts + i]
        )
        for i in range(parts)
    ]
    for c in loads + loads2:
        c.start()
    own = jnp.zeros((feats, nodes), F32)
    both = jnp.zeros((feats, nodes), F32)
    for i in range(parts):
        loads[i].wait()
        got = wide(got_ref, i * each, (i + 1) * each, 0, feats)
        code = codes_v[i * span : (i + 1) * span]
        both = both + jnp.dot(got, code, preferred_element_type=F32)
        own = own + jnp.dot(got, split_codes(code, own_w), preferred_element_type=F32)
    summed = ((both - own_w * own) / fanout).astype(BF16)
    pre = jnp.dot(ws_ref[...], own.astype(BF16), preferred_element_type=F32)
    pre = pre + jnp.dot(wn_ref[...], summed, preferred_element_type=F32) + b_ref[...]
    hidden = jnp.maximum(pre, 0.0).astype(BF16)
    terms = jnp.dot(w2_ref[...], hidden, preferred_element_type=F32).astype(BF16)
    for i in range(parts):
        loads2[i].wait()
        part = jnp.dot(terms, choose_v[:, i * span2 : (i + 1) * span2], preferred_element_type=F32).astype(BF16)
        for r in range(each):
            out_ref[i * each + r] = part[:, r * cap2 : (r + 1) * cap2]


def layer(got, code, chosen, w1_self, w1_neigh, bias1, w2, fanout, cap):
    blocks = got.shape[0]
    parts = 8
    return pl.pallas_call(
        functools.partial(layer_kernel, fanout, parts),
        out_shape=jax.ShapeDtypeStruct((blocks, w2.shape[0], cap), BF16),
        in_specs=[WHOLE_VMEM, IN_HBM, IN_HBM] + [WHOLE_VMEM] * 4,
        out_specs=WHOLE_VMEM,
        scratch_shapes=[
            pltpu.VMEM(code.shape, BF16),
            pltpu.VMEM(chosen.shape, BF16),
            pltpu.SemaphoreType.DMA((2 * parts,)),
        ],
        compiler_params=params(40),
        name="layer",
    )(got, code, chosen, w1_self, w1_neigh, bias1[:, None], w2)


def logits_kernel(fanout, got_ref, code_ref, b_ref, out_ref):
    blocks, half = got_ref.shape[0], got_ref.shape[1] // 2
    classes = out_ref.shape[0]
    own_w = own_weight(fanout)
    code = code_ref[...]
    own = split_codes(code, own_w)
    mine = jnp.dot(wide(got_ref, 0, blocks, 0, half), own, preferred_element_type=F32)
    near = jnp.dot(wide(got_ref, 0, blocks, half, 2 * half), code - own_w * own, preferred_element_type=F32) / fanout
    out_ref[...] = (mine + near)[:classes] + b_ref[...]


def final(got, code, bias2, fanout):
    return pl.pallas_call(
        functools.partial(logits_kernel, fanout),
        out_shape=jax.ShapeDtypeStruct((bias2.shape[0], code.shape[1]), F32),
        in_specs=[WHOLE_VMEM] * 3,
        out_specs=WHOLE_VMEM,
        compiler_params=params(20),
        name="logits",
    )(got, code, bias2[:, None])


def mask_rows(received, counts, capacity):
    is_live = (jnp.arange(capacity, dtype=jnp.int32)[None, :] < counts[:, None]).reshape(-1)
    flat = received.reshape(-1, received.shape[-1])
    return jnp.where(is_live[:, None], flat, jnp.zeros((), flat.dtype))


def right_product(rows, weight):
    return lax.dot_general(
        rows, weight, (((1,), (1,)), ((), ())), preferred_element_type=jnp.float32
    )


def plain_body(
    table_t,
    req_rows,
    count1,
    frontier_list,
    req2_rows,
    count2,
    seed_list,
    w1_self,
    w1_neigh,
    bias1,
    w2_self,
    w2_neigh,
    bias2,
):
    feat_width = table_t.shape[0]
    capacity = req_rows.shape[1]
    table_rows = table_t.T
    picked_rows = jnp.take(
        table_rows,
        lax.all_to_all(req_rows, AXES, split_axis=0, concat_axis=0, tiled=True),
        axis=0,
    )
    received = lax.all_to_all(
        picked_rows, AXES, split_axis=0, concat_axis=0, tiled=True
    )
    flat = mask_rows(received, count1, capacity)
    fanout_two = frontier_list.shape[0] - 1
    front_nodes = frontier_list.shape[1]
    picked = jnp.take(flat, frontier_list.reshape(-1), axis=0).reshape(
        fanout_two + 1, front_nodes, feat_width
    )
    summed = (jnp.sum(picked[1:].astype(jnp.float32), axis=0) / fanout_two).astype(jnp.bfloat16)
    preact = right_product(picked[0], w1_self) + right_product(summed, w1_neigh) + bias1[None, :]
    hidden_rows = jax.nn.relu(preact).astype(jnp.bfloat16)
    cap_two = req2_rows.shape[1]
    payload = jnp.concatenate(
        [right_product(hidden_rows, w2_self), right_product(hidden_rows, w2_neigh)], axis=1
    )
    chosen = jnp.take(
        payload,
        lax.all_to_all(req2_rows, AXES, split_axis=0, concat_axis=0, tiled=True),
        axis=0,
    )
    got_back = lax.all_to_all(chosen, AXES, split_axis=0, concat_axis=0, tiled=True)
    flat_two = mask_rows(got_back, count2, cap_two)
    fanout_one = seed_list.shape[0] - 1
    seed_nodes = seed_list.shape[1]
    picked_two = jnp.take(flat_two, seed_list.reshape(-1), axis=0).reshape(
        fanout_one + 1, seed_nodes, flat_two.shape[1]
    )
    classes = w2_self.shape[0]
    near = jnp.sum(picked_two[1:, :, classes:], axis=0) / fanout_one
    logits = (picked_two[0, :, :classes] + near).T + bias2[:, None]
    return logits


MOST = 8 << 20


def body(
    table_t,
    req_rows,
    count1,
    frontier_list,
    req2_rows,
    count2,
    seed_list,
    w1_self,
    w1_neigh,
    bias1,
    w2_self,
    w2_neigh,
    bias2,
):
    cap = req_rows.shape[1]
    fits = req_rows.size * frontier_list.shape[1] <= MOST and req2_rows.shape[1] == cap
    if not fits or table_t.shape[1] > 32768 or frontier_list.shape[1] > 65536:
        return plain_body(
            table_t,
            req_rows,
            count1,
            frontier_list,
            req2_rows,
            count2,
            seed_list,
            w1_self,
            w1_neigh,
            bias1,
            w2_self,
            w2_neigh,
            bias2,
        )
    asked = exchange(req_rows * 65536 + req2_rows)
    got1 = exchange(fetch(asked, table_t))
    code1 = codes(count1, frontier_list, cap, pltpu.HBM)
    chosen = choose(asked, frontier_list.shape[1])
    classes = w2_self.shape[0]
    half = -(-classes // 16) * 16
    pad = ((0, half - classes), (0, 0))
    w2 = jnp.concatenate([jnp.pad(w2_self, pad), jnp.pad(w2_neigh, pad)], axis=0)
    out2 = layer(got1, code1, chosen, w1_self, w1_neigh, bias1, w2, frontier_list.shape[0] - 1, cap)
    got2 = exchange(out2)
    code2 = codes(count2, seed_list, cap, jax.ShapeDtypeStruct)
    return final(got2, code2, bias2, seed_list.shape[0] - 1)


def solution(mesh):
    split, split1 = P(AXES, None), P(AXES)
    cols = P(None, AXES)
    in_specs = (cols, split, split1, cols, split, split1, cols, P(), P(), P(), P(), P(), P())
    return jax.shard_map(body, mesh=mesh, in_specs=in_specs, out_specs=cols, check_vma=False)
```

```python
import functools

import jax
import jax.numpy as jnp
from jax import lax
from jax.experimental import pallas as pl
from jax.experimental.pallas import tpu as pltpu
from jax.sharding import PartitionSpec as P

AXES = ("shard", "grp")
F32 = jnp.float32
BF16 = jnp.bfloat16
I32 = jnp.int32
WHOLE_VMEM = pl.BlockSpec(memory_space=pltpu.VMEM)
WHOLE_SMEM = pl.BlockSpec(memory_space=pltpu.SMEM)
IN_HBM = pl.BlockSpec(memory_space=pltpu.HBM)


def exchange(blocks):
    return lax.all_to_all(blocks, AXES, split_axis=0, concat_axis=0, tiled=True)


def params(mib):
    return pltpu.CompilerParams(vmem_limit_bytes=mib << 20)


def identity(n, dtype):
    rows = lax.broadcasted_iota(I32, (n, n), 0)
    lanes = lax.broadcasted_iota(I32, (n, n), 1)
    return jnp.where(rows == lanes, 1.0, 0.0).astype(dtype)


def fetch_kernel(
    parts, ahead, group, idx_ref, asked_hbm, table_hbm, out_hbm, cols, rows, even, odd, slots, out_v, asked_v, sems, out_sems, slot_sems
):
    feats, n = cols.shape
    blocks, rows_out, cap = out_v.shape
    span = n // parts
    loads = [
        pltpu.make_async_copy(
            table_hbm.at[:, pl.ds(i * span, span)], cols.at[:, pl.ds(i * span, span)], sems.at[i]
        )
        for i in range(parts)
    ]
    for c in loads[:ahead]:
        c.start()

    def refill(slot, first):
        return pltpu.make_async_copy(idx_ref.at[pl.ds(first, group)], slots[slot], slot_sems.at[slot])

    refill(0, 0).start()
    refill(1, group).start()
    ask = pltpu.make_async_copy(asked_hbm, asked_v, sems.at[parts])
    ask.start()
    wide = max(w for w in range(1, 9) if (span // 128) % w == 0)
    for i in range(parts):
        if i + ahead < parts:
            loads[i + ahead].start()
        loads[i].wait()

        def tile(t, _):
            for u in range(wide):
                at = pl.multiple_of(i * span + (t * wide + u) * 128, 128)
                rows[pl.ds(at, 128), :feats] = cols[:, pl.ds(at, 128)].astype(F32).T
            return 0

        lax.fori_loop(0, span // 128 // wide, tile, 0, unroll=True)

    ask.wait()
    base = feats // 16 * 16
    row = lax.broadcasted_iota(I32, (16, cap), 0)

    def gather(slot, u, buf):
        for j in range(cap):
            buf[pl.ds(j, 1), :] = rows[pl.ds(slots[slot][u, j], 1), :]

    def turn(r, buf):
        y = buf[...].T
        asked = asked_v[pl.ds(r, 1), :]
        high, low = (asked // cap).astype(F32), (asked % cap).astype(F32)
        tail = jnp.where(row == feats - base, high, jnp.where(row == feats - base + 1, low, y[base : base + 16]))
        out_v[r, :base] = y[:base].astype(BF16)
        out_v[r, base:] = tail[: rows_out - base].astype(BF16)

    def leave(i):
        return pltpu.make_async_copy(out_v.at[pl.ds(i * group, group)], out_hbm.at[pl.ds(i * group, group)], out_sems.at[i])

    trips = blocks // (2 * group)

    def many(i, _):
        for slot in range(2):
            first = (2 * i + slot) * group
            refill(slot, first).wait()
            for u in range(group):
                buf = (even, odd)[u % 2]
                gather(slot, u, buf)
                turn(first + u, buf)

            @pl.when(i + 1 < trips)
            def _():
                refill(slot, first + 2 * group).start()

            leave(2 * i + slot).start()
        return 0

    lax.fori_loop(0, trips, many, 0)
    for i in range(2 * trips):
        leave(i).wait()


def fetch(idx, asked, table_t):
    feats, n = table_t.shape
    blocks, cap = idx.shape
    parts = 8 if n % 1024 == 0 else 1
    group = 4
    return pl.pallas_call(
        functools.partial(fetch_kernel, parts, parts, group),
        out_shape=pltpu.HBM((blocks, feats + 2, cap), BF16),
        in_specs=[WHOLE_VMEM, IN_HBM, IN_HBM],
        out_specs=IN_HBM,
        scratch_shapes=[
            pltpu.VMEM((feats, n), BF16),
            pltpu.VMEM((n, 128), F32),
            pltpu.VMEM((cap, 128), F32),
            pltpu.VMEM((cap, 128), F32),
            [pltpu.SMEM((group, cap), I32), pltpu.SMEM((group, cap), I32)],
            pltpu.VMEM((blocks, feats + 2, cap), BF16),
            pltpu.VMEM((blocks, cap), I32),
            pltpu.SemaphoreType.DMA((parts + 1,)),
            pltpu.SemaphoreType.DMA((blocks // group,)),
            pltpu.SemaphoreType.DMA((2,)),
        ],
        compiler_params=params(40),
        name="fetch",
    )(idx, pltpu.with_memory_space_constraint(asked, pltpu.HBM), pltpu.with_memory_space_constraint(table_t, pltpu.HBM))


def own_weight(fanout):
    return 1 << fanout.bit_length()


def codes_kernel(own, cap, count_ref, list_ref, out_ref):
    depth, width = list_ref.shape
    each = out_ref.shape[1] // cap
    zero = jnp.zeros((16, width), BF16)
    hit = [jnp.full((16, width), own if k == 0 else 1, BF16) for k in range(2)]

    def step(t, _):
        o = pl.program_id(1) * each + t
        local = list_ref[...] - o * cap
        live = (local >= 0) & (local < count_ref[o])
        local = jnp.where(live, local, -1).astype(F32)
        want = [jnp.broadcast_to(local[k : k + 1], (16, width)).astype(BF16) for k in range(depth)]
        for g in range(cap // 16):
            slot = (lax.broadcasted_iota(I32, (16, width), 0) + g * 16).astype(F32).astype(BF16)
            total = jnp.where(want[0] == slot, hit[0], zero)
            for k in range(1, depth):
                total = total + jnp.where(want[k] == slot, hit[1], zero)
            out_ref[0, pl.ds(pl.multiple_of(t * cap + g * 16, 16), 16), :] = total
        return 0

    lax.fori_loop(0, each, step, 0)


def codes(counts, lists, cap, place):
    depth, nodes = lists.shape
    blocks = counts.shape[0]
    width = 256
    each = 8
    return pl.pallas_call(
        functools.partial(codes_kernel, own_weight(depth - 1), cap),
        grid=(nodes // width, blocks // each),
        out_shape=place((nodes // width, blocks * cap, width), BF16),
        in_specs=[WHOLE_SMEM, pl.BlockSpec((depth, width), lambda q, o: (0, q))],
        out_specs=pl.BlockSpec((1, each * cap, width), lambda q, o: (q, o, 0)),
        compiler_params=params(8),
        name="codes",
    )(counts, lists)


def split_codes(code, own):
    return jnp.where(code >= own, jnp.ones((), BF16), jnp.zeros((), BF16))


def layer_kernel(
    fanout, got_ref, first_ref, codes_hbm, ws_ref, wn_ref, b_ref, w2_ref, out_v, codes_v, got_v, choose_v, terms_v, sems
):
    blocks, _, cap = got_ref.shape
    feats = got_v.shape[0]
    rest, slots, width = codes_v.shape
    parts = rest + 1
    pairs, nodes, _ = choose_v.shape
    own_w = own_weight(fanout)
    def load(q):
        return pltpu.make_async_copy(codes_hbm.at[q], codes_v.at[q], sems.at[q])

    for q in range(rest):
        load(q).start()
    one, zero = jnp.ones((16, cap), BF16), jnp.zeros((16, cap), BF16)

    def choose(p, _):
        for u in range(2):
            o = 2 * p + u
            got_v[:, pl.ds(pl.multiple_of(o * cap, cap), cap)] = got_ref[o, :feats]
            asked = got_ref[o, feats : feats + 2].astype(F32)
            asked = asked[0:1] * cap + asked[1:2]
            for base in range(0, nodes, 256):
                local = asked - base
                local = jnp.where((local >= 0) & (local < 256), local, -1.0)
                want = jnp.broadcast_to(local, (16, cap)).astype(BF16)
                for g in range(0, 256, 16):
                    node = (lax.broadcasted_iota(I32, (16, cap), 0) + g).astype(F32).astype(BF16)
                    choose_v[p, base + g : base + g + 16, u * cap : (u + 1) * cap] = jnp.where(want == node, one, zero)
        return 0

    lax.fori_loop(0, pairs, choose, 0)
    for q in range(parts):
        if q:
            load(q - 1).wait()
        code = codes_v[q - 1] if q else first_ref[0]
        both = jnp.dot(got_v[...], code, preferred_element_type=F32)
        own = jnp.dot(got_v[...], split_codes(code, own_w), preferred_element_type=F32)
        summed = ((both - own_w * own) / fanout).astype(BF16)
        pre = jnp.dot(ws_ref[...], own.astype(BF16), preferred_element_type=F32)
        pre = pre + jnp.dot(wn_ref[...], summed, preferred_element_type=F32) + b_ref[...]
        hidden = jnp.maximum(pre, 0.0).astype(BF16)
        terms = jnp.dot(w2_ref[...], hidden, preferred_element_type=F32)
        terms_v[:, q * width : (q + 1) * width] = terms.astype(BF16)

    def send(i, _):
        for u in range(2):
            p = 2 * i + u
            part = jnp.dot(terms_v[...], choose_v[p], preferred_element_type=F32).astype(BF16)
            out_v[2 * p] = part[:, :cap]
            out_v[2 * p + 1] = part[:, cap:]
        return 0

    lax.fori_loop(0, pairs // 2, send, 0, unroll=True)


def layer(got, first, code, w1_self, w1_neigh, bias1, w2, fanout):
    blocks, _, cap = got.shape
    rest, slots, width = code.shape
    nodes = (rest + 1) * width
    return pl.pallas_call(
        functools.partial(layer_kernel, fanout),
        out_shape=pltpu.HBM((blocks, w2.shape[0], cap), BF16),
        in_specs=[WHOLE_VMEM, WHOLE_VMEM, IN_HBM] + [WHOLE_VMEM] * 4,
        out_specs=WHOLE_VMEM,
        scratch_shapes=[
            pltpu.VMEM(code.shape, BF16),
            pltpu.VMEM((w1_self.shape[1], slots), BF16),
            pltpu.VMEM((blocks // 2, nodes, 2 * cap), BF16),
            pltpu.VMEM((w2.shape[0], nodes), BF16),
            pltpu.SemaphoreType.DMA((rest,)),
        ],
        compiler_params=params(40),
        name="layer",
    )(got, first, pltpu.with_memory_space_constraint(code, pltpu.HBM), w1_self, w1_neigh, bias1[:, None], w2)


def wide(ref, first, last, lo, hi):
    return jnp.concatenate([ref[o, lo:hi] for o in range(first, last)], axis=1)


def logits_kernel(fanout, got_ref, code_ref, b_ref, out_ref):
    blocks, half = got_ref.shape[0], got_ref.shape[1] // 2
    classes = out_ref.shape[0]
    own_w = own_weight(fanout)
    code = code_ref[0]
    own = split_codes(code, own_w)
    mine = jnp.dot(wide(got_ref, 0, blocks, 0, half), own, preferred_element_type=F32)
    near = jnp.dot(wide(got_ref, 0, blocks, half, 2 * half), code - own_w * own, preferred_element_type=F32) / fanout
    out_ref[...] = (mine + near)[:classes] + b_ref[...]


def final(got, code, bias2, fanout):
    return pl.pallas_call(
        functools.partial(logits_kernel, fanout),
        out_shape=jax.ShapeDtypeStruct((bias2.shape[0], code.shape[2]), F32),
        in_specs=[WHOLE_VMEM] * 3,
        out_specs=WHOLE_VMEM,
        compiler_params=params(20),
        name="logits",
    )(got, code, bias2[:, None])


def mask_rows(received, counts, capacity):
    is_live = (jnp.arange(capacity, dtype=jnp.int32)[None, :] < counts[:, None]).reshape(-1)
    flat = received.reshape(-1, received.shape[-1])
    return jnp.where(is_live[:, None], flat, jnp.zeros((), flat.dtype))


def right_product(rows, weight):
    return lax.dot_general(
        rows, weight, (((1,), (1,)), ((), ())), preferred_element_type=jnp.float32
    )


def plain_body(
    table_t,
    req_rows,
    count1,
    frontier_list,
    req2_rows,
    count2,
    seed_list,
    w1_self,
    w1_neigh,
    bias1,
    w2_self,
    w2_neigh,
    bias2,
):
    feat_width = table_t.shape[0]
    capacity = req_rows.shape[1]
    table_rows = table_t.T
    picked_rows = jnp.take(
        table_rows,
        lax.all_to_all(req_rows, AXES, split_axis=0, concat_axis=0, tiled=True),
        axis=0,
    )
    received = lax.all_to_all(
        picked_rows, AXES, split_axis=0, concat_axis=0, tiled=True
    )
    flat = mask_rows(received, count1, capacity)
    fanout_two = frontier_list.shape[0] - 1
    front_nodes = frontier_list.shape[1]
    picked = jnp.take(flat, frontier_list.reshape(-1), axis=0).reshape(
        fanout_two + 1, front_nodes, feat_width
    )
    summed = (jnp.sum(picked[1:].astype(jnp.float32), axis=0) / fanout_two).astype(jnp.bfloat16)
    preact = right_product(picked[0], w1_self) + right_product(summed, w1_neigh) + bias1[None, :]
    hidden_rows = jax.nn.relu(preact).astype(jnp.bfloat16)
    cap_two = req2_rows.shape[1]
    payload = jnp.concatenate(
        [right_product(hidden_rows, w2_self), right_product(hidden_rows, w2_neigh)], axis=1
    )
    chosen = jnp.take(
        payload,
        lax.all_to_all(req2_rows, AXES, split_axis=0, concat_axis=0, tiled=True),
        axis=0,
    )
    got_back = lax.all_to_all(chosen, AXES, split_axis=0, concat_axis=0, tiled=True)
    flat_two = mask_rows(got_back, count2, cap_two)
    fanout_one = seed_list.shape[0] - 1
    seed_nodes = seed_list.shape[1]
    picked_two = jnp.take(flat_two, seed_list.reshape(-1), axis=0).reshape(
        fanout_one + 1, seed_nodes, flat_two.shape[1]
    )
    classes = w2_self.shape[0]
    near = jnp.sum(picked_two[1:, :, classes:], axis=0) / fanout_one
    logits = (picked_two[0, :, :classes] + near).T + bias2[:, None]
    return logits


MOST = 8 << 20


def body(
    table_t,
    req_rows,
    count1,
    frontier_list,
    req2_rows,
    count2,
    seed_list,
    w1_self,
    w1_neigh,
    bias1,
    w2_self,
    w2_neigh,
    bias2,
):
    cap = req_rows.shape[1]
    fits = req_rows.size * frontier_list.shape[1] <= MOST and req2_rows.shape[1] == cap
    if not fits or table_t.shape[1] > 32768 or frontier_list.shape[1] > 65536:
        return plain_body(
            table_t,
            req_rows,
            count1,
            frontier_list,
            req2_rows,
            count2,
            seed_list,
            w1_self,
            w1_neigh,
            bias1,
            w2_self,
            w2_neigh,
            bias2,
        )
    idx = exchange(req_rows)
    got1 = exchange(fetch(idx, req2_rows, table_t))
    first = codes(count1, frontier_list[:, :256], cap, jax.ShapeDtypeStruct)
    code1 = codes(count1, frontier_list[:, 256:], cap, pltpu.HBM)
    classes = w2_self.shape[0]
    half = -(-classes // 16) * 16
    pad = ((0, half - classes), (0, 0))
    w2 = jnp.concatenate([jnp.pad(w2_self, pad), jnp.pad(w2_neigh, pad)], axis=0)
    out2 = layer(got1, first, code1, w1_self, w1_neigh, bias1, w2, frontier_list.shape[0] - 1)
    got2 = exchange(out2)
    code2 = codes(count2, seed_list, cap, jax.ShapeDtypeStruct)
    return final(got2, code2, bias2, seed_list.shape[0] - 1)


def solution(mesh):
    split, split1 = P(AXES, None), P(AXES)
    cols = P(None, AXES)
    in_specs = (cols, split, split1, cols, split, split1, cols, P(), P(), P(), P(), P(), P())
    return jax.shard_map(body, mesh=mesh, in_specs=in_specs, out_specs=cols, check_vma=False)
```

```python
import functools

import jax
import jax.numpy as jnp
from jax import lax
from jax.experimental import pallas as pl
from jax.experimental.pallas import tpu as pltpu
from jax.sharding import PartitionSpec as P

AXES = ("shard", "grp")
F32 = jnp.float32
BF16 = jnp.bfloat16
I32 = jnp.int32
WHOLE_VMEM = pl.BlockSpec(memory_space=pltpu.VMEM)
WHOLE_SMEM = pl.BlockSpec(memory_space=pltpu.SMEM)
IN_HBM = pl.BlockSpec(memory_space=pltpu.HBM)


def exchange(blocks):
    return lax.all_to_all(blocks, AXES, split_axis=0, concat_axis=0, tiled=True)


def params(mib):
    return pltpu.CompilerParams(vmem_limit_bytes=mib << 20)


def identity(n, dtype):
    rows = lax.broadcasted_iota(I32, (n, n), 0)
    lanes = lax.broadcasted_iota(I32, (n, n), 1)
    return jnp.where(rows == lanes, 1.0, 0.0).astype(dtype)


def fetch_kernel(
    parts, ahead, group, idx_ref, extra_hbm, table_hbm, out_hbm, cols, rows, even, odd, slots, out_v, extra_v, sems, out_sems, slot_sems
):
    feats, n = cols.shape
    blocks, rows_out, cap = out_v.shape
    span = n // parts
    loads = [
        pltpu.make_async_copy(
            table_hbm.at[:, pl.ds(i * span, span)], cols.at[:, pl.ds(i * span, span)], sems.at[i]
        )
        for i in range(parts)
    ]
    for c in loads[:ahead]:
        c.start()

    def refill(slot, first):
        return pltpu.make_async_copy(idx_ref.at[pl.ds(first, group)], slots[slot], slot_sems.at[slot])

    refill(0, 0).start()
    refill(1, group).start()
    ask = pltpu.make_async_copy(extra_hbm, extra_v, sems.at[parts])
    ask.start()
    wide = max(w for w in range(1, 9) if (span // 128) % w == 0)
    for i in range(parts):
        if i + ahead < parts:
            loads[i + ahead].start()
        loads[i].wait()

        def tile(t, _):
            for u in range(wide):
                at = pl.multiple_of(i * span + (t * wide + u) * 128, 128)
                rows[pl.ds(at, 128), :feats] = cols[:, pl.ds(at, 128)].astype(F32).T
            return 0

        lax.fori_loop(0, span // 128 // wide, tile, 0, unroll=True)

    ask.wait()
    base = feats // 8 * 8
    row = lax.broadcasted_iota(I32, (8, cap), 0)

    def gather(slot, u, buf):
        for j in range(cap):
            buf[pl.ds(j, 1), :] = rows[pl.ds(slots[slot][u, j], 1), :]

    def turn(r, buf):
        y = buf[...].T
        out_v[r, :base] = y[:base].astype(BF16)
        out_v[r, base:] = jnp.where(row < feats - base, y[base : base + 8], extra_v[r]).astype(BF16)

    def leave(i):
        return pltpu.make_async_copy(out_v.at[pl.ds(i * group, group)], out_hbm.at[pl.ds(i * group, group)], out_sems.at[i])

    trips = blocks // (2 * group)

    def many(i, _):
        for slot in range(2):
            first = (2 * i + slot) * group
            refill(slot, first).wait()
            for u in range(group):
                buf = (even, odd)[u % 2]
                gather(slot, u, buf)
                turn(first + u, buf)

            @pl.when(i + 1 < trips)
            def _():
                refill(slot, first + 2 * group).start()

            leave(2 * i + slot).start()
        return 0

    lax.fori_loop(0, trips, many, 0)
    for i in range(2 * trips):
        leave(i).wait()


def fetch(idx, extra, table_t):
    feats, n = table_t.shape
    blocks, cap = idx.shape
    parts = 8 if n % 1024 == 0 else 1
    group = 4
    return pl.pallas_call(
        functools.partial(fetch_kernel, parts, parts, group),
        out_shape=pltpu.HBM((blocks, feats + 4, cap), BF16),
        in_specs=[WHOLE_VMEM, IN_HBM, IN_HBM],
        out_specs=IN_HBM,
        scratch_shapes=[
            pltpu.VMEM((feats, n), BF16),
            pltpu.VMEM((n, 128), F32),
            pltpu.VMEM((cap, 128), F32),
            pltpu.VMEM((cap, 128), F32),
            [pltpu.SMEM((group, cap), I32), pltpu.SMEM((group, cap), I32)],
            pltpu.VMEM((blocks, feats + 4, cap), BF16),
            pltpu.VMEM((blocks, 8, cap), F32),
            pltpu.SemaphoreType.DMA((parts + 1,)),
            pltpu.SemaphoreType.DMA((blocks // group,)),
            pltpu.SemaphoreType.DMA((2,)),
        ],
        compiler_params=params(40),
        name="fetch",
    )(idx, pltpu.with_memory_space_constraint(extra, pltpu.HBM), pltpu.with_memory_space_constraint(table_t, pltpu.HBM))


PARTS = 6


def room_of(cap):
    return cap // PARTS


def lane_part(shape, cap):
    lane = lax.broadcasted_iota(I32, shape, len(shape) - 1)
    part = lane // room_of(cap)
    return jnp.where(part < PARTS, part, -1), lane % room_of(cap)


def ask_kernel(off, req2_ref, seeds_ref, extra_ref, rank_ref):
    blocks, cap = req2_ref.shape
    own = seeds_ref[0:1, :]
    seeds = own.shape[1]
    room = room_of(cap)
    owner, slot = own // cap, own % cap

    def bits(mask):
        return jnp.where(mask, 1.0, 0.0).astype(BF16)

    mine = bits(lax.broadcasted_iota(I32, (blocks, seeds), 0) == owner)
    before = bits(lax.broadcasted_iota(I32, (seeds, seeds), 0) < lax.broadcasted_iota(I32, (seeds, seeds), 1))
    mine32 = mine.astype(F32)
    rank = jnp.sum(mine32 * jnp.dot(mine, before, preferred_element_type=F32), axis=0, keepdims=True)
    rank_ref[...] = rank
    at_slot = bits(lax.broadcasted_iota(I32, (cap, seeds), 0) == slot)
    lane = lax.broadcasted_iota(I32, (cap, seeds), 0)
    entry = jnp.where(lane // room < PARTS, lane % room, -1).astype(F32)
    at_rank = bits(entry == rank)
    full = jnp.max(jnp.where(rank >= room, 1.0, 0.0))
    last = lax.broadcasted_iota(I32, (blocks, cap), 1) == cap - 1
    extra_ref[...] = jnp.zeros_like(extra_ref)
    for k, part in enumerate((req2_ref[...] // cap, req2_ref[...] % cap)):
        part = part.astype(F32)
        extra_ref[:, off + k, :] = part
        node = jnp.dot(part.astype(BF16), at_slot, preferred_element_type=F32) * mine32
        listed = lax.dot_general(node.astype(BF16), at_rank, (((1,), (1,)), ((), ())), preferred_element_type=F32)
        extra_ref[:, off + 2 + k, :] = jnp.where(last, full, listed)


def ask(req2_rows, seed_list, feats):
    blocks, cap = req2_rows.shape
    return pl.pallas_call(
        functools.partial(ask_kernel, feats % 8),
        out_shape=(
            jax.ShapeDtypeStruct((blocks, 8, cap), F32),
            jax.ShapeDtypeStruct((1, seed_list.shape[1]), F32),
        ),
        in_specs=[WHOLE_VMEM, WHOLE_VMEM],
        out_specs=(WHOLE_VMEM, WHOLE_VMEM),
        compiler_params=params(8),
        name="ask",
    )(req2_rows, seed_list)


def own_weight(fanout):
    return 1 << fanout.bit_length()


def codes_kernel(own, cap, count_ref, list_ref, out_ref):
    depth, width = list_ref.shape
    each = out_ref.shape[1] // cap
    zero = jnp.zeros((16, width), BF16)
    hit = [jnp.full((16, width), own if k == 0 else 1, BF16) for k in range(2)]

    def step(t, _):
        o = pl.program_id(1) * each + t
        local = list_ref[...] - o * cap
        live = (local >= 0) & (local < count_ref[o])
        local = jnp.where(live, local, -1).astype(F32)
        want = [jnp.broadcast_to(local[k : k + 1], (16, width)).astype(BF16) for k in range(depth)]
        for g in range(cap // 16):
            slot = (lax.broadcasted_iota(I32, (16, width), 0) + g * 16).astype(F32).astype(BF16)
            total = jnp.where(want[0] == slot, hit[0], zero)
            for k in range(1, depth):
                total = total + jnp.where(want[k] == slot, hit[1], zero)
            out_ref[0, pl.ds(pl.multiple_of(t * cap + g * 16, 16), 16), :] = total
        return 0

    lax.fori_loop(0, each, step, 0)


def codes(counts, lists, cap, place):
    depth, nodes = lists.shape
    blocks = counts.shape[0]
    width = 256
    each = 8
    return pl.pallas_call(
        functools.partial(codes_kernel, own_weight(depth - 1), cap),
        grid=(nodes // width, blocks // each),
        out_shape=place((nodes // width, blocks * cap, width), BF16),
        in_specs=[WHOLE_SMEM, pl.BlockSpec((depth, width), lambda q, o: (0, q))],
        out_specs=pl.BlockSpec((1, each * cap, width), lambda q, o: (q, o, 0)),
        compiler_params=params(8),
        name="codes",
    )(counts, lists)


def rank_codes_kernel(own, cap, count_ref, list_ref, rank_ref, out_ref):
    depth, width = list_ref.shape
    each = out_ref.shape[0] // cap
    zero = jnp.zeros((16, width), BF16)
    hit = [jnp.full((16, width), v, BF16) for v in (own, 1)]

    def step(t, _):
        o = pl.program_id(0) * each + t
        local = list_ref[...] - o * cap
        live = (local >= 0) & (local < count_ref[o])
        local = jnp.where(live, local, -1).astype(F32)
        rank = jnp.where(live[0:1], rank_ref[...], -cap * 1.0)
        rank = jnp.where(rank < room_of(cap), rank, -cap * 1.0)
        rows = [rank + q * room_of(cap) for q in range(PARTS)] + [local[k : k + 1] for k in range(1, depth)]
        want = [jnp.broadcast_to(row, (16, width)).astype(BF16) for row in rows]
        for g in range(cap // 16):
            slot = (lax.broadcasted_iota(I32, (16, width), 0) + g * 16).astype(F32).astype(BF16)
            total = jnp.where(want[0] == slot, hit[0], zero)
            for k in range(1, len(rows)):
                total = total + jnp.where(want[k] == slot, hit[k >= PARTS], zero)
            out_ref[pl.ds(pl.multiple_of(t * cap + g * 16, 16), 16), :] = total
        return 0

    lax.fori_loop(0, each, step, 0)


def rank_codes(counts, lists, rank, cap):
    depth, seeds = lists.shape
    blocks = counts.shape[0]
    each = 8
    return pl.pallas_call(
        functools.partial(rank_codes_kernel, own_weight(depth - 1), cap),
        grid=(blocks // each,),
        out_shape=jax.ShapeDtypeStruct((blocks * cap, seeds), BF16),
        in_specs=[WHOLE_SMEM, WHOLE_VMEM, WHOLE_VMEM],
        out_specs=pl.BlockSpec((each * cap, seeds), lambda o: (o, 0)),
        compiler_params=params(8),
        name="rank_codes",
    )(counts, lists, rank)


def split_codes(code, own):
    return jnp.where(code >= own, jnp.ones((), BF16), jnp.zeros((), BF16))


def layer_kernel(
    fanout, got_ref, first_ref, codes_hbm, ws_ref, wn_ref, b_ref, w2_ref, out_v, terms_ref, flag_ref, codes_v, got_v, choose_v, terms_v, sems
):
    blocks, _, cap = got_ref.shape
    feats = got_v.shape[0]
    rest, slots, width = codes_v.shape
    parts = rest + 1
    pairs, nodes = blocks // 2, choose_v.shape[1]
    chunks = -(-blocks // PARTS)
    half = w2_ref.shape[0] // 2
    deep = half // PARTS
    own_w = own_weight(fanout)
    def load(q):
        return pltpu.make_async_copy(codes_hbm.at[q], codes_v.at[q], sems.at[q])

    for q in range(rest):
        load(q).start()
    one, zero = jnp.ones((16, cap), BF16), jnp.zeros((16, cap), BF16)

    def fill(asked, p, u):
        for base in range(0, nodes, 256):
            local = asked - base
            local = jnp.where((local >= 0) & (local < 256), local, -1.0)
            want = jnp.broadcast_to(local, (16, cap)).astype(BF16)
            for g in range(0, 256, 16):
                node = (lax.broadcasted_iota(I32, (16, cap), 0) + g).astype(F32).astype(BF16)
                choose_v[p, base + g : base + g + 16, u * cap : (u + 1) * cap] = jnp.where(want == node, one, zero)

    def asked_of(o, row):
        asked = got_ref[o, feats : feats + 4].astype(F32)
        return asked[row : row + 1] * cap + asked[row + 1 : row + 2]

    def choose(p, _):
        for u in range(2):
            o = 2 * p + u
            got_v[:, pl.ds(pl.multiple_of(o * cap, cap), cap)] = got_ref[o, :feats]
            fill(asked_of(o, 0), p, u)
        return 0

    lax.fori_loop(0, pairs, choose, 0)
    part, _ = lane_part((1, cap), cap)
    for c in range(chunks):
        asked = jnp.full((1, cap), -1.0, F32)
        for u in range(min(PARTS, blocks - c * PARTS)):
            asked = jnp.where(part == u, asked_of(c * PARTS + u, 2), asked)
        fill(asked, pairs + c // 2, c % 2)
    flag = got_ref[0, feats + 2 : feats + 3].astype(F32)
    for o in range(1, blocks):
        flag = jnp.maximum(flag, got_ref[o, feats + 2 : feats + 3].astype(F32))
    flag_ref[...] = flag
    for q in range(parts):
        if q:
            load(q - 1).wait()
        code = codes_v[q - 1] if q else first_ref[0]
        both = jnp.dot(got_v[...], code, preferred_element_type=F32)
        own = jnp.dot(got_v[...], split_codes(code, own_w), preferred_element_type=F32)
        summed = ((both - own_w * own) / fanout).astype(BF16)
        pre = jnp.dot(ws_ref[...], own.astype(BF16), preferred_element_type=F32)
        pre = pre + jnp.dot(wn_ref[...], summed, preferred_element_type=F32) + b_ref[...]
        hidden = jnp.maximum(pre, 0.0).astype(BF16)
        terms = jnp.dot(w2_ref[...], hidden, preferred_element_type=F32)
        terms_v[:, q * width : (q + 1) * width] = terms.astype(BF16)

    terms_ref[...] = terms_v[:half]
    part8, _ = lane_part((deep, cap), cap)
    for p in range(pairs, choose_v.shape[0]):
        found = jnp.dot(terms_v[:half], choose_v[p], preferred_element_type=F32)
        for v in range(2):
            c = 2 * (p - pairs) + v
            for u in range(max(0, min(PARTS, blocks - c * PARTS))):
                block = jnp.zeros((deep, cap), F32)
                for q in range(PARTS):
                    piece = found[q * deep : (q + 1) * deep, v * cap : (v + 1) * cap]
                    piece = pltpu.roll(piece, (q - u) * room_of(cap) % cap, 1)
                    block = jnp.where(part8 == q, piece, block)
                out_v[c * PARTS + u, half:] = block.astype(BF16)
    for p in range(pairs):
        near = jnp.dot(terms_v[half:], choose_v[p], preferred_element_type=F32).astype(BF16)
        out_v[2 * p, :half] = near[:, :cap]
        out_v[2 * p + 1, :half] = near[:, cap:]


def layer(got, first, code, w1_self, w1_neigh, bias1, w2, fanout):
    blocks, _, cap = got.shape
    rest, slots, width = code.shape
    nodes = (rest + 1) * width
    half = w2.shape[0] // 2
    return pl.pallas_call(
        functools.partial(layer_kernel, fanout),
        out_shape=(
            pltpu.HBM((blocks, half + half // PARTS, cap), BF16),
            pltpu.HBM((half, nodes), BF16),
            jax.ShapeDtypeStruct((1, cap), F32),
        ),
        in_specs=[WHOLE_VMEM, WHOLE_VMEM, IN_HBM] + [WHOLE_VMEM] * 4,
        out_specs=(WHOLE_VMEM,) * 3,
        scratch_shapes=[
            pltpu.VMEM(code.shape, BF16),
            pltpu.VMEM((w1_self.shape[1], slots), BF16),
            pltpu.VMEM((blocks // 2 + -(-blocks // (2 * PARTS)), nodes, 2 * cap), BF16),
            pltpu.VMEM((w2.shape[0], nodes), BF16),
            pltpu.SemaphoreType.DMA((rest,)),
        ],
        compiler_params=params(40),
        name="layer",
    )(got, first, pltpu.with_memory_space_constraint(code, pltpu.HBM), w1_self, w1_neigh, bias1[:, None], w2)


def wide(ref, first, last, lo, hi):
    return jnp.concatenate([ref[o, lo:hi] for o in range(first, last)], axis=1)


def logits_kernel(fanout, got_ref, code_ref, b_ref, out_ref):
    blocks, half = got_ref.shape[0], got_ref.shape[1] // 2
    classes = out_ref.shape[0]
    own_w = own_weight(fanout)
    code = code_ref[0]
    own = split_codes(code, own_w)
    mine = jnp.dot(wide(got_ref, 0, blocks, 0, half), own, preferred_element_type=F32)
    near = jnp.dot(wide(got_ref, 0, blocks, half, 2 * half), code - own_w * own, preferred_element_type=F32) / fanout
    out_ref[...] = (mine + near)[:classes] + b_ref[...]


def final(got, code, bias2, fanout):
    return pl.pallas_call(
        functools.partial(logits_kernel, fanout),
        out_shape=jax.ShapeDtypeStruct((bias2.shape[0], code.shape[2]), F32),
        in_specs=[WHOLE_VMEM] * 3,
        out_specs=WHOLE_VMEM,
        compiler_params=params(20),
        name="logits",
    )(got, code, bias2[:, None])


def mask_rows(received, counts, capacity):
    is_live = (jnp.arange(capacity, dtype=jnp.int32)[None, :] < counts[:, None]).reshape(-1)
    flat = received.reshape(-1, received.shape[-1])
    return jnp.where(is_live[:, None], flat, jnp.zeros((), flat.dtype))


def right_product(rows, weight):
    return lax.dot_general(
        rows, weight, (((1,), (1,)), ((), ())), preferred_element_type=jnp.float32
    )


def plain_body(
    table_t,
    req_rows,
    count1,
    frontier_list,
    req2_rows,
    count2,
    seed_list,
    w1_self,
    w1_neigh,
    bias1,
    w2_self,
    w2_neigh,
    bias2,
):
    feat_width = table_t.shape[0]
    capacity = req_rows.shape[1]
    table_rows = table_t.T
    picked_rows = jnp.take(
        table_rows,
        lax.all_to_all(req_rows, AXES, split_axis=0, concat_axis=0, tiled=True),
        axis=0,
    )
    received = lax.all_to_all(
        picked_rows, AXES, split_axis=0, concat_axis=0, tiled=True
    )
    flat = mask_rows(received, count1, capacity)
    fanout_two = frontier_list.shape[0] - 1
    front_nodes = frontier_list.shape[1]
    picked = jnp.take(flat, frontier_list.reshape(-1), axis=0).reshape(
        fanout_two + 1, front_nodes, feat_width
    )
    summed = (jnp.sum(picked[1:].astype(jnp.float32), axis=0) / fanout_two).astype(jnp.bfloat16)
    preact = right_product(picked[0], w1_self) + right_product(summed, w1_neigh) + bias1[None, :]
    hidden_rows = jax.nn.relu(preact).astype(jnp.bfloat16)
    cap_two = req2_rows.shape[1]
    payload = jnp.concatenate(
        [right_product(hidden_rows, w2_self), right_product(hidden_rows, w2_neigh)], axis=1
    )
    chosen = jnp.take(
        payload,
        lax.all_to_all(req2_rows, AXES, split_axis=0, concat_axis=0, tiled=True),
        axis=0,
    )
    got_back = lax.all_to_all(chosen, AXES, split_axis=0, concat_axis=0, tiled=True)
    flat_two = mask_rows(got_back, count2, cap_two)
    fanout_one = seed_list.shape[0] - 1
    seed_nodes = seed_list.shape[1]
    picked_two = jnp.take(flat_two, seed_list.reshape(-1), axis=0).reshape(
        fanout_one + 1, seed_nodes, flat_two.shape[1]
    )
    classes = w2_self.shape[0]
    near = jnp.sum(picked_two[1:, :, classes:], axis=0) / fanout_one
    logits = (picked_two[0, :, :classes] + near).T + bias2[:, None]
    return logits


def rank_logits_kernel(fanout, got_ref, code_ref, b_ref, out_ref):
    blocks, rows, cap = got_ref.shape
    deep = rows // (PARTS + 1)
    half = rows - deep
    own_w = own_weight(fanout)
    code = code_ref[...]
    own = split_codes(code, own_w)
    part, _ = lane_part((deep, cap), cap)

    def spread(o):
        terms = got_ref[o, half:].astype(F32)
        return jnp.concatenate([jnp.where(part == q, terms, 0.0) for q in range(PARTS)], axis=0).astype(BF16)

    mine = jnp.dot(jnp.concatenate([spread(o) for o in range(blocks)], axis=1), own, preferred_element_type=F32)
    near = jnp.dot(wide(got_ref, 0, blocks, 0, half), code - own_w * own, preferred_element_type=F32) / fanout
    out_ref[...] = (mine + near)[: out_ref.shape[0]] + b_ref[...]


def rank_final(got, code, bias2, fanout):
    return pl.pallas_call(
        functools.partial(rank_logits_kernel, fanout),
        out_shape=pltpu.HBM((bias2.shape[0], code.shape[1]), F32),
        in_specs=[WHOLE_VMEM] * 3,
        out_specs=WHOLE_VMEM,
        compiler_params=params(20),
        name="rank_logits",
    )(got, code, bias2[:, None])


MOST = 8 << 20


def body(
    table_t,
    req_rows,
    count1,
    frontier_list,
    req2_rows,
    count2,
    seed_list,
    w1_self,
    w1_neigh,
    bias1,
    w2_self,
    w2_neigh,
    bias2,
):
    cap = req_rows.shape[1]
    fits = req_rows.size * frontier_list.shape[1] <= MOST and req2_rows.shape[1] == cap and table_t.shape[0] % 8 == 4
    if not fits or table_t.shape[1] > 32768 or frontier_list.shape[1] > 65536:
        return plain_body(
            table_t,
            req_rows,
            count1,
            frontier_list,
            req2_rows,
            count2,
            seed_list,
            w1_self,
            w1_neigh,
            bias1,
            w2_self,
            w2_neigh,
            bias2,
        )
    feats, fanout_two, fanout_one = table_t.shape[0], frontier_list.shape[0] - 1, seed_list.shape[0] - 1
    extra, rank = ask(req2_rows, seed_list, feats)
    got1 = exchange(fetch(exchange(req_rows), extra, table_t))
    first = codes(count1, frontier_list[:, :256], cap, jax.ShapeDtypeStruct)
    code1 = codes(count1, frontier_list[:, 256:], cap, pltpu.HBM)
    classes = w2_self.shape[0]
    half = -(-classes // 48) * 48
    pad = ((0, half - classes), (0, 0))
    w2 = jnp.concatenate([jnp.pad(w2_self, pad), jnp.pad(w2_neigh, pad)], axis=0)
    out2, terms, flag = layer(got1, first, code1, w1_self, w1_neigh, bias1, w2, fanout_two)
    got2 = exchange(out2)
    logits = rank_final(got2, rank_codes(count2, seed_list, rank, cap), bias2, fanout_one)

    def in_full(logits):
        asked = exchange(req2_rows)
        own = jnp.take(terms, asked.reshape(-1), axis=1, mode="clip").reshape(half, -1, cap).transpose(1, 0, 2)
        got = jnp.concatenate([exchange(own), got2[:, :half]], axis=1)
        return final(got, codes(count2, seed_list, cap, jax.ShapeDtypeStruct), bias2, fanout_one)

    return lax.cond(flag[0, cap - 1] > 0.5, in_full, lambda logits: logits, logits)


def solution(mesh):
    split, split1 = P(AXES, None), P(AXES)
    cols = P(None, AXES)
    in_specs = (cols, split, split1, cols, split, split1, cols, P(), P(), P(), P(), P(), P())
    return jax.shard_map(body, mesh=mesh, in_specs=in_specs, out_specs=cols, check_vma=False)
```

```python
import functools

import jax
import jax.numpy as jnp
from jax import lax
from jax.experimental import pallas as pl
from jax.experimental.pallas import tpu as pltpu
from jax.sharding import PartitionSpec as P

AXES = ("shard", "grp")
F32 = jnp.float32
BF16 = jnp.bfloat16
I32 = jnp.int32
WHOLE_VMEM = pl.BlockSpec(memory_space=pltpu.VMEM)
WHOLE_SMEM = pl.BlockSpec(memory_space=pltpu.SMEM)
IN_HBM = pl.BlockSpec(memory_space=pltpu.HBM)


def exchange(blocks):
    return lax.all_to_all(blocks, AXES, split_axis=0, concat_axis=0, tiled=True)


def params(mib):
    return pltpu.CompilerParams(vmem_limit_bytes=mib << 20)


def identity(n, dtype):
    rows = lax.broadcasted_iota(I32, (n, n), 0)
    lanes = lax.broadcasted_iota(I32, (n, n), 1)
    return jnp.where(rows == lanes, 1.0, 0.0).astype(dtype)


def head_kernel(parts, table_hbm, out_ref, cols, sems):
    feats, n = cols.shape
    span = n // parts
    loads = [
        pltpu.make_async_copy(table_hbm.at[:, pl.ds(i * span, span)], cols.at[:, pl.ds(i * span, span)], sems.at[i])
        for i in range(parts)
    ]
    for c in loads:
        c.start()
    for i in range(parts):
        loads[i].wait()
        for at in range(i * span, (i + 1) * span, 128):
            out_ref[at : at + 128, :feats] = cols[:, at : at + 128].T.astype(F32)


def head_rows(table_t, n):
    feats = table_t.shape[0]
    return pl.pallas_call(
        functools.partial(head_kernel, 4),
        out_shape=jax.ShapeDtypeStruct((n, 128), F32),
        in_specs=[IN_HBM],
        out_specs=WHOLE_VMEM,
        scratch_shapes=[pltpu.VMEM((feats, n), BF16), pltpu.SemaphoreType.DMA((4,))],
        compiler_params=params(16),
        name="head_rows",
    )(pltpu.with_memory_space_constraint(table_t, pltpu.HBM))


def fetch_kernel(
    parts, group, idx_ref, head_ref, extra_hbm, table_hbm, out_hbm, cols, rows, bufs, idx_s, out_v, extra_v, sems, out_sems
):
    feats, n = cols.shape
    head = head_ref.shape[0]
    blocks, rows_out, cap = out_v.shape
    span = n // parts
    loads = [
        pltpu.make_async_copy(
            table_hbm.at[:, pl.ds(head + i * span, span)], cols.at[:, pl.ds(i * span, span)], sems.at[i]
        )
        for i in range(parts)
    ]
    for c in loads:
        c.start()

    to_scalar = pltpu.make_async_copy(idx_ref, idx_s, sems.at[parts + 1])
    to_scalar.start()
    ask = pltpu.make_async_copy(extra_hbm, extra_v, sems.at[parts])
    ask.start()
    take = pltpu.make_async_copy(head_ref, rows.at[pl.ds(0, head)], sems.at[parts + 2])
    take.start()
    for i in range(parts):
        loads[i].wait()
        for at in range(i * span, (i + 1) * span, 128):
            rows[head + at : head + at + 128, :feats] = cols[:, at : at + 128].T.astype(F32)

    take.wait()
    to_scalar.wait()
    ask.wait()
    base = feats // 8 * 8
    row = lax.broadcasted_iota(I32, (8, cap), 0)

    def gather(r, buf):
        for j in range(cap):
            buf[pl.ds(j, 1), :] = rows[pl.ds(idx_s[r, j], 1), :]

    def turn(r, buf):
        y = buf[...].T
        out_v[r, :base] = y[:base].astype(BF16)
        out_v[r, base:] = jnp.where(row < feats - base, y[base : base + 8], extra_v[r]).astype(BF16)

    def leave(i):
        return pltpu.make_async_copy(out_v.at[pl.ds(i * group, group)], out_hbm.at[pl.ds(i * group, group)], out_sems.at[i])

    for r in range(blocks):
        gather(r, bufs[r % len(bufs)])
        if r:
            turn(r - 1, bufs[(r - 1) % len(bufs)])
        if r and r % group == 0:
            leave(r // group - 1).start()
    turn(blocks - 1, bufs[(blocks - 1) % len(bufs)])
    leave(blocks // group - 1).start()
    for i in range(blocks // group):
        leave(i).wait()


def fetch(idx, extra, table_t, head):
    feats, n = table_t.shape
    left = n - head.shape[0]
    blocks, cap = idx.shape
    parts = max(p for p in range(1, 9) if left // 128 % p == 0)
    group = 4
    return pl.pallas_call(
        functools.partial(fetch_kernel, parts, group),
        out_shape=pltpu.HBM((blocks, feats + 4, cap), BF16),
        in_specs=[WHOLE_VMEM, WHOLE_VMEM, IN_HBM, IN_HBM],
        out_specs=IN_HBM,
        scratch_shapes=[
            pltpu.VMEM((feats, left), BF16),
            pltpu.VMEM((n, 128), F32),
            [pltpu.VMEM((cap, 128), F32) for _ in range(4)],
            pltpu.SMEM((blocks, cap), I32),
            pltpu.VMEM((blocks, feats + 4, cap), BF16),
            pltpu.VMEM((blocks, 8, cap), F32),
            pltpu.SemaphoreType.DMA((parts + 3,)),
            pltpu.SemaphoreType.DMA((blocks // group,)),
        ],
        compiler_params=params(40),
        name="fetch",
    )(idx, head, pltpu.with_memory_space_constraint(extra, pltpu.HBM), pltpu.with_memory_space_constraint(table_t, pltpu.HBM))


PARTS = 6


def room_of(cap):
    return cap // PARTS


def lane_part(shape, cap):
    lane = lax.broadcasted_iota(I32, shape, len(shape) - 1)
    part = lane // room_of(cap)
    return jnp.where(part < PARTS, part, -1), lane % room_of(cap)


def ask_kernel(off, req2_ref, seeds_ref, extra_ref, rank_ref):
    blocks, cap = req2_ref.shape
    own = seeds_ref[0:1, :]
    seeds = own.shape[1]
    room = room_of(cap)
    owner, slot = own // cap, own % cap

    def bits(mask):
        return jnp.where(mask, 1.0, 0.0).astype(BF16)

    mine = bits(lax.broadcasted_iota(I32, (blocks, seeds), 0) == owner)
    before = bits(lax.broadcasted_iota(I32, (seeds, seeds), 0) < lax.broadcasted_iota(I32, (seeds, seeds), 1))
    mine32 = mine.astype(F32)
    rank = jnp.sum(mine32 * jnp.dot(mine, before, preferred_element_type=F32), axis=0, keepdims=True)
    rank_ref[...] = rank
    at_slot = bits(lax.broadcasted_iota(I32, (cap, seeds), 0) == slot)
    lane = lax.broadcasted_iota(I32, (cap, seeds), 0)
    entry = jnp.where(lane // room < PARTS, lane % room, -1).astype(F32)
    at_rank = bits(entry == rank)
    full = jnp.max(jnp.where(rank >= room, 1.0, 0.0))
    last = lax.broadcasted_iota(I32, (blocks, cap), 1) == cap - 1
    extra_ref[...] = jnp.zeros_like(extra_ref)
    for k, part in enumerate((req2_ref[...] // cap, req2_ref[...] % cap)):
        part = part.astype(F32)
        extra_ref[:, off + k, :] = part
        node = jnp.dot(part.astype(BF16), at_slot, preferred_element_type=F32) * mine32
        listed = lax.dot_general(node.astype(BF16), at_rank, (((1,), (1,)), ((), ())), preferred_element_type=F32)
        extra_ref[:, off + 2 + k, :] = jnp.where(last, full, listed)


def ask(req2_rows, seed_list, feats):
    blocks, cap = req2_rows.shape
    return pl.pallas_call(
        functools.partial(ask_kernel, feats % 8),
        out_shape=(
            pltpu.HBM((blocks, 8, cap), F32),
            jax.ShapeDtypeStruct((1, seed_list.shape[1]), F32),
        ),
        in_specs=[WHOLE_VMEM, WHOLE_VMEM],
        out_specs=(WHOLE_VMEM, WHOLE_VMEM),
        compiler_params=params(8),
        name="ask",
    )(req2_rows, seed_list)


def own_weight(fanout):
    return 1 << fanout.bit_length()


def codes_kernel(own, cap, count_ref, list_ref, out_ref):
    depth, width = list_ref.shape
    each = out_ref.shape[1] // cap
    zero = jnp.zeros((16, width), BF16)
    hit = [jnp.full((16, width), own if k == 0 else 1, BF16) for k in range(2)]

    def step(t, _):
        o = pl.program_id(1) * each + t
        local = list_ref[...] - o * cap
        live = (local >= 0) & (local < count_ref[o])
        local = jnp.where(live, local, -1).astype(F32)
        want = [jnp.broadcast_to(local[k : k + 1], (16, width)).astype(BF16) for k in range(depth)]
        for g in range(cap // 16):
            slot = (lax.broadcasted_iota(I32, (16, width), 0) + g * 16).astype(F32).astype(BF16)
            total = jnp.where(want[0] == slot, hit[0], zero)
            for k in range(1, depth):
                total = total + jnp.where(want[k] == slot, hit[1], zero)
            out_ref[0, pl.ds(pl.multiple_of(t * cap + g * 16, 16), 16), :] = total
        return 0

    lax.fori_loop(0, each, step, 0)


def codes(counts, lists, cap, place):
    depth, nodes = lists.shape
    blocks = counts.shape[0]
    width = 256
    each = 8
    return pl.pallas_call(
        functools.partial(codes_kernel, own_weight(depth - 1), cap),
        grid=(nodes // width, blocks // each),
        out_shape=place((nodes // width, blocks * cap, width), BF16),
        in_specs=[WHOLE_SMEM, pl.BlockSpec((depth, width), lambda q, o: (0, q))],
        out_specs=pl.BlockSpec((1, each * cap, width), lambda q, o: (q, o, 0)),
        compiler_params=params(8),
        name="codes",
    )(counts, lists)


def rank_codes_kernel(own, cap, count_ref, list_ref, rank_ref, out_ref):
    depth, width = list_ref.shape
    each = out_ref.shape[0] // cap
    zero = jnp.zeros((16, width), BF16)
    hit = [jnp.full((16, width), v, BF16) for v in (own, 1)]

    def step(t, _):
        o = pl.program_id(0) * each + t
        local = list_ref[...] - o * cap
        live = (local >= 0) & (local < count_ref[o])
        local = jnp.where(live, local, -1).astype(F32)
        rank = jnp.where(live[0:1], rank_ref[...], -cap * 1.0)
        rank = jnp.where(rank < room_of(cap), rank, -cap * 1.0)
        rows = [rank + q * room_of(cap) for q in range(PARTS)] + [local[k : k + 1] for k in range(1, depth)]
        want = [jnp.broadcast_to(row, (16, width)).astype(BF16) for row in rows]
        for g in range(cap // 16):
            slot = (lax.broadcasted_iota(I32, (16, width), 0) + g * 16).astype(F32).astype(BF16)
            total = jnp.where(want[0] == slot, hit[0], zero)
            for k in range(1, len(rows)):
                total = total + jnp.where(want[k] == slot, hit[k >= PARTS], zero)
            out_ref[pl.ds(pl.multiple_of(t * cap + g * 16, 16), 16), :] = total
        return 0

    lax.fori_loop(0, each, step, 0)


def rank_codes(counts, lists, rank, cap):
    depth, seeds = lists.shape
    blocks = counts.shape[0]
    each = 8
    return pl.pallas_call(
        functools.partial(rank_codes_kernel, own_weight(depth - 1), cap),
        grid=(blocks // each,),
        out_shape=jax.ShapeDtypeStruct((blocks * cap, seeds), BF16),
        in_specs=[WHOLE_SMEM, WHOLE_VMEM, WHOLE_VMEM],
        out_specs=pl.BlockSpec((each * cap, seeds), lambda o: (o, 0)),
        compiler_params=params(8),
        name="rank_codes",
    )(counts, lists, rank)


def split_codes(code, own):
    return jnp.where(code >= own, jnp.ones((), BF16), jnp.zeros((), BF16))


def layer_kernel(
    fanout, got_ref, first_ref, codes_hbm, ws_ref, wn_ref, b_ref, w2_ref, out_v, terms_ref, flag_ref, codes_v, got_v, choose_v, terms_v, sems
):
    blocks, _, cap = got_ref.shape
    feats = got_v.shape[0]
    rest, slots, width = codes_v.shape
    parts = rest + 1
    pairs, nodes = blocks // 2, choose_v.shape[1]
    half = w2_ref.shape[0] // 2
    deep = half // PARTS
    own_w = own_weight(fanout)
    def load(q):
        return pltpu.make_async_copy(codes_hbm.at[q], codes_v.at[q], sems.at[q])

    for q in range(rest):
        load(q).start()
    one, zero = jnp.ones((16, 2 * cap), BF16), jnp.zeros((16, 2 * cap), BF16)

    def fill(asked, p):
        for base in range(0, nodes, 256):
            local = asked - base
            local = jnp.where((local >= 0) & (local < 256), local, -1.0)
            want = jnp.broadcast_to(local, (16, 2 * cap)).astype(BF16)
            for g in range(0, 256, 16):
                node = (lax.broadcasted_iota(I32, (16, 2 * cap), 0) + g).astype(F32).astype(BF16)
                choose_v[p, base + g : base + g + 16, :] = jnp.where(want == node, one, zero)

    def asked_of(o, row):
        asked = got_ref[o, feats : feats + 4].astype(F32)
        return asked[row : row + 1] * cap + asked[row + 1 : row + 2]

    def choose(p, _):
        for u in range(2):
            o = 2 * p + u
            got_v[:, pl.ds(pl.multiple_of(o * cap, cap), cap)] = got_ref[o, :feats]
        fill(jnp.concatenate([asked_of(2 * p, 0), asked_of(2 * p + 1, 0)], axis=1), p)
        return 0

    lax.fori_loop(0, pairs, choose, 0)
    part, _ = lane_part((1, cap), cap)
    for p in range(pairs, choose_v.shape[0]):
        both = []
        for c in (2 * (p - pairs), 2 * (p - pairs) + 1):
            asked = jnp.full((1, cap), -1.0, F32)
            for u in range(max(0, min(PARTS, blocks - c * PARTS))):
                asked = jnp.where(part == u, asked_of(c * PARTS + u, 2), asked)
            both.append(asked)
        fill(jnp.concatenate(both, axis=1), p)
    flag = got_ref[0, feats + 2 : feats + 3].astype(F32)
    for o in range(1, blocks):
        flag = jnp.maximum(flag, got_ref[o, feats + 2 : feats + 3].astype(F32))
    flag_ref[...] = flag
    for q in range(parts):
        if q == 1:
            for k in range(rest):
                load(k).wait()
        code = codes_v[q - 1] if q else first_ref[0]
        both = jnp.dot(got_v[...], code, preferred_element_type=F32)
        own = jnp.dot(got_v[...], split_codes(code, own_w), preferred_element_type=F32)
        summed = ((both - own_w * own) / fanout).astype(BF16)
        pre = jnp.dot(ws_ref[...], own.astype(BF16), preferred_element_type=F32)
        pre = pre + jnp.dot(wn_ref[...], summed, preferred_element_type=F32) + b_ref[...]
        hidden = jnp.maximum(pre, 0.0).astype(BF16)
        terms = jnp.dot(w2_ref[...], hidden, preferred_element_type=F32)
        terms_v[:, q * width : (q + 1) * width] = terms.astype(BF16)

    terms_ref[...] = terms_v[:half]
    part8, _ = lane_part((deep, cap), cap)
    for p in range(pairs, choose_v.shape[0]):
        found = jnp.dot(terms_v[:half], choose_v[p], preferred_element_type=F32)
        for v in range(2):
            c = 2 * (p - pairs) + v
            for u in range(max(0, min(PARTS, blocks - c * PARTS))):
                block = jnp.zeros((deep, cap), F32)
                for q in range(PARTS):
                    piece = found[q * deep : (q + 1) * deep, v * cap : (v + 1) * cap]
                    piece = pltpu.roll(piece, (q - u) * room_of(cap) % cap, 1)
                    block = jnp.where(part8 == q, piece, block)
                out_v[c * PARTS + u, half:] = block.astype(BF16)
    for p in range(pairs):
        near = jnp.dot(terms_v[half:], choose_v[p], preferred_element_type=F32).astype(BF16)
        out_v[2 * p, :half] = near[:, :cap]
        out_v[2 * p + 1, :half] = near[:, cap:]


def layer(got, first, code, w1_self, w1_neigh, bias1, w2, fanout):
    blocks, _, cap = got.shape
    rest, slots, width = code.shape
    nodes = (rest + 1) * width
    half = w2.shape[0] // 2
    return pl.pallas_call(
        functools.partial(layer_kernel, fanout),
        out_shape=(
            pltpu.HBM((blocks, half + half // PARTS, cap), BF16),
            pltpu.HBM((half, nodes), BF16),
            jax.ShapeDtypeStruct((1, cap), F32),
        ),
        in_specs=[WHOLE_VMEM, WHOLE_VMEM, IN_HBM] + [WHOLE_VMEM] * 4,
        out_specs=(WHOLE_VMEM,) * 3,
        scratch_shapes=[
            pltpu.VMEM(code.shape, BF16),
            pltpu.VMEM((w1_self.shape[1], slots), BF16),
            pltpu.VMEM((blocks // 2 + -(-blocks // (2 * PARTS)), nodes, 2 * cap), BF16),
            pltpu.VMEM((w2.shape[0], nodes), BF16),
            pltpu.SemaphoreType.DMA((rest,)),
        ],
        compiler_params=params(40),
        name="layer",
    )(got, first, pltpu.with_memory_space_constraint(code, pltpu.HBM), w1_self, w1_neigh, bias1[:, None], w2)


def wide(ref, first, last, lo, hi):
    return jnp.concatenate([ref[o, lo:hi] for o in range(first, last)], axis=1)


def logits_kernel(fanout, got_ref, code_ref, b_ref, out_ref):
    blocks, half = got_ref.shape[0], got_ref.shape[1] // 2
    classes = out_ref.shape[0]
    own_w = own_weight(fanout)
    code = code_ref[0]
    own = split_codes(code, own_w)
    mine = jnp.dot(wide(got_ref, 0, blocks, 0, half), own, preferred_element_type=F32)
    near = jnp.dot(wide(got_ref, 0, blocks, half, 2 * half), code - own_w * own, preferred_element_type=F32) / fanout
    out_ref[...] = (mine + near)[:classes] + b_ref[...]


def final(got, code, bias2, fanout):
    return pl.pallas_call(
        functools.partial(logits_kernel, fanout),
        out_shape=jax.ShapeDtypeStruct((bias2.shape[0], code.shape[2]), F32),
        in_specs=[WHOLE_VMEM] * 3,
        out_specs=WHOLE_VMEM,
        compiler_params=params(20),
        name="logits",
    )(got, code, bias2[:, None])


def mask_rows(received, counts, capacity):
    is_live = (jnp.arange(capacity, dtype=jnp.int32)[None, :] < counts[:, None]).reshape(-1)
    flat = received.reshape(-1, received.shape[-1])
    return jnp.where(is_live[:, None], flat, jnp.zeros((), flat.dtype))


def right_product(rows, weight):
    return lax.dot_general(
        rows, weight, (((1,), (1,)), ((), ())), preferred_element_type=jnp.float32
    )


def plain_body(
    table_t,
    req_rows,
    count1,
    frontier_list,
    req2_rows,
    count2,
    seed_list,
    w1_self,
    w1_neigh,
    bias1,
    w2_self,
    w2_neigh,
    bias2,
):
    feat_width = table_t.shape[0]
    capacity = req_rows.shape[1]
    table_rows = table_t.T
    picked_rows = jnp.take(
        table_rows,
        lax.all_to_all(req_rows, AXES, split_axis=0, concat_axis=0, tiled=True),
        axis=0,
    )
    received = lax.all_to_all(
        picked_rows, AXES, split_axis=0, concat_axis=0, tiled=True
    )
    flat = mask_rows(received, count1, capacity)
    fanout_two = frontier_list.shape[0] - 1
    front_nodes = frontier_list.shape[1]
    picked = jnp.take(flat, frontier_list.reshape(-1), axis=0).reshape(
        fanout_two + 1, front_nodes, feat_width
    )
    summed = (jnp.sum(picked[1:].astype(jnp.float32), axis=0) / fanout_two).astype(jnp.bfloat16)
    preact = right_product(picked[0], w1_self) + right_product(summed, w1_neigh) + bias1[None, :]
    hidden_rows = jax.nn.relu(preact).astype(jnp.bfloat16)
    cap_two = req2_rows.shape[1]
    payload = jnp.concatenate(
        [right_product(hidden_rows, w2_self), right_product(hidden_rows, w2_neigh)], axis=1
    )
    chosen = jnp.take(
        payload,
        lax.all_to_all(req2_rows, AXES, split_axis=0, concat_axis=0, tiled=True),
        axis=0,
    )
    got_back = lax.all_to_all(chosen, AXES, split_axis=0, concat_axis=0, tiled=True)
    flat_two = mask_rows(got_back, count2, cap_two)
    fanout_one = seed_list.shape[0] - 1
    seed_nodes = seed_list.shape[1]
    picked_two = jnp.take(flat_two, seed_list.reshape(-1), axis=0).reshape(
        fanout_one + 1, seed_nodes, flat_two.shape[1]
    )
    classes = w2_self.shape[0]
    near = jnp.sum(picked_two[1:, :, classes:], axis=0) / fanout_one
    logits = (picked_two[0, :, :classes] + near).T + bias2[:, None]
    return logits


def rank_logits_kernel(fanout, got_ref, code_ref, b_ref, out_ref):
    blocks, rows, cap = got_ref.shape
    deep = rows // (PARTS + 1)
    half = rows - deep
    own_w = own_weight(fanout)
    code = code_ref[...]
    own = split_codes(code, own_w)
    part, _ = lane_part((deep, cap), cap)

    def spread(o):
        terms = got_ref[o, half:].astype(F32)
        return jnp.concatenate([jnp.where(part == q, terms, 0.0) for q in range(PARTS)], axis=0).astype(BF16)

    mine = jnp.dot(jnp.concatenate([spread(o) for o in range(blocks)], axis=1), own, preferred_element_type=F32)
    near = jnp.dot(wide(got_ref, 0, blocks, 0, half), code - own_w * own, preferred_element_type=F32) / fanout
    out_ref[...] = (mine + near)[: out_ref.shape[0]] + b_ref[...]


def rank_final(got, code, bias2, fanout):
    return pl.pallas_call(
        functools.partial(rank_logits_kernel, fanout),
        out_shape=pltpu.HBM((bias2.shape[0], code.shape[1]), F32),
        in_specs=[WHOLE_VMEM] * 3,
        out_specs=WHOLE_VMEM,
        compiler_params=params(20),
        name="rank_logits",
    )(got, code, bias2[:, None])


HEAD = 6144
MOST = 8 << 20


def body(
    table_t,
    req_rows,
    count1,
    frontier_list,
    req2_rows,
    count2,
    seed_list,
    w1_self,
    w1_neigh,
    bias1,
    w2_self,
    w2_neigh,
    bias2,
):
    cap = req_rows.shape[1]
    fits = req_rows.size * frontier_list.shape[1] <= MOST and req2_rows.shape[1] == cap and table_t.shape[0] % 8 == 4
    fits = fits and table_t.shape[1] % 128 == 0 and table_t.shape[1] > HEAD
    if not fits or table_t.shape[1] > 32768 or frontier_list.shape[1] > 65536:
        return plain_body(
            table_t,
            req_rows,
            count1,
            frontier_list,
            req2_rows,
            count2,
            seed_list,
            w1_self,
            w1_neigh,
            bias1,
            w2_self,
            w2_neigh,
            bias2,
        )
    feats, fanout_two, fanout_one = table_t.shape[0], frontier_list.shape[0] - 1, seed_list.shape[0] - 1
    extra, rank = ask(req2_rows, seed_list, feats)
    got1 = exchange(fetch(exchange(req_rows), extra, table_t, head_rows(table_t, HEAD)))
    first = codes(count1, frontier_list[:, :256], cap, jax.ShapeDtypeStruct)
    code1 = codes(count1, frontier_list[:, 256:], cap, pltpu.HBM)
    classes = w2_self.shape[0]
    half = -(-classes // 48) * 48
    pad = ((0, half - classes), (0, 0))
    w2 = jnp.concatenate([jnp.pad(w2_self, pad), jnp.pad(w2_neigh, pad)], axis=0)
    out2, terms, flag = layer(got1, first, code1, w1_self, w1_neigh, bias1, w2, fanout_two)
    got2 = exchange(out2)
    logits = rank_final(got2, rank_codes(count2, seed_list, rank, cap), bias2, fanout_one)

    def in_full(logits):
        asked = exchange(req2_rows)
        own = jnp.take(terms, asked.reshape(-1), axis=1, mode="clip").reshape(half, -1, cap).transpose(1, 0, 2)
        got = jnp.concatenate([exchange(own), got2[:, :half]], axis=1)
        return final(got, codes(count2, seed_list, cap, jax.ShapeDtypeStruct), bias2, fanout_one)

    return lax.cond(flag[0, cap - 1] > 0.5, in_full, lambda logits: logits, logits)


def solution(mesh):
    split, split1 = P(AXES, None), P(AXES)
    cols = P(None, AXES)
    in_specs = (cols, split, split1, cols, split, split1, cols, P(), P(), P(), P(), P(), P())
    return jax.shard_map(body, mesh=mesh, in_specs=in_specs, out_specs=cols, check_vma=False)
```

```python
import functools

import jax
import jax.numpy as jnp
from jax import lax
from jax.experimental import pallas as pl
from jax.experimental.pallas import tpu as pltpu
from jax.sharding import PartitionSpec as P

AXES = ("shard", "grp")
F32 = jnp.float32
BF16 = jnp.bfloat16
I32 = jnp.int32
WHOLE_VMEM = pl.BlockSpec(memory_space=pltpu.VMEM)
WHOLE_SMEM = pl.BlockSpec(memory_space=pltpu.SMEM)
IN_HBM = pl.BlockSpec(memory_space=pltpu.HBM)


def exchange(blocks):
    return lax.all_to_all(blocks, AXES, split_axis=0, concat_axis=0, tiled=True)


def params(mib):
    return pltpu.CompilerParams(vmem_limit_bytes=mib << 20)


def identity(n, dtype):
    rows = lax.broadcasted_iota(I32, (n, n), 0)
    lanes = lax.broadcasted_iota(I32, (n, n), 1)
    return jnp.where(rows == lanes, 1.0, 0.0).astype(dtype)


def head_kernel(parts, table_hbm, out_ref, cols, sems):
    feats, n = cols.shape
    span = n // parts
    loads = [
        pltpu.make_async_copy(table_hbm.at[:, pl.ds(i * span, span)], cols.at[:, pl.ds(i * span, span)], sems.at[i])
        for i in range(parts)
    ]
    for c in loads:
        c.start()
    for i in range(parts):
        loads[i].wait()
        for at in range(i * span, (i + 1) * span, 128):
            out_ref[at : at + 128, :feats] = cols[:, at : at + 128].T.astype(F32)


def head_rows(table_t, n):
    feats = table_t.shape[0]
    return pl.pallas_call(
        functools.partial(head_kernel, 4),
        out_shape=jax.ShapeDtypeStruct((n, 128), F32),
        in_specs=[IN_HBM],
        out_specs=WHOLE_VMEM,
        scratch_shapes=[pltpu.VMEM((feats, n), BF16), pltpu.SemaphoreType.DMA((4,))],
        compiler_params=params(16),
        name="head_rows",
    )(pltpu.with_memory_space_constraint(table_t, pltpu.HBM))


def fetch_kernel(
    parts, group, idx_ref, head_ref, extra_hbm, table_hbm, out_hbm, cols, rows, bufs, idx_s, out_v, extra_v, sems, out_sems
):
    feats, n = cols.shape
    head = head_ref.shape[0]
    blocks, rows_out, cap = out_v.shape
    span = n // parts
    loads = [
        pltpu.make_async_copy(
            table_hbm.at[:, pl.ds(head + i * span, span)], cols.at[:, pl.ds(i * span, span)], sems.at[i]
        )
        for i in range(parts)
    ]
    for c in loads:
        c.start()

    to_scalar = pltpu.make_async_copy(idx_ref, idx_s, sems.at[parts + 1])
    to_scalar.start()
    ask = pltpu.make_async_copy(extra_hbm, extra_v, sems.at[parts])
    ask.start()
    take = pltpu.make_async_copy(head_ref, rows.at[pl.ds(0, head)], sems.at[parts + 2])
    take.start()
    for i in range(parts):
        loads[i].wait()
        for at in range(i * span, (i + 1) * span, 128):
            rows[head + at : head + at + 128, :feats] = cols[:, at : at + 128].T.astype(F32)

    take.wait()
    to_scalar.wait()
    ask.wait()
    base = feats // 8 * 8
    row = lax.broadcasted_iota(I32, (8, cap), 0)

    def gather(r, buf):
        for j in range(cap):
            buf[pl.ds(j, 1), :] = rows[pl.ds(idx_s[r, j], 1), :]

    def turn(r, buf):
        y = buf[...].T
        out_v[r, :base] = y[:base].astype(BF16)
        out_v[r, base:] = jnp.where(row < feats - base, y[base : base + 8], extra_v[r]).astype(BF16)

    def leave(i):
        return pltpu.make_async_copy(out_v.at[pl.ds(i * group, group)], out_hbm.at[pl.ds(i * group, group)], out_sems.at[i])

    for r in range(blocks + 1):
        if r < blocks:
            gather(r, bufs[r % len(bufs)])
        done = r - 1
        if done >= 0:
            turn(done, bufs[done % len(bufs)])
            if done % group == group - 1:
                leave(done // group).start()
    for i in range(blocks // group):
        leave(i).wait()


def fetch(idx, extra, table_t, head):
    feats, n = table_t.shape
    left = n - head.shape[0]
    blocks, cap = idx.shape
    parts = max(p for p in range(1, 9) if left // 128 % p == 0)
    group = 4
    return pl.pallas_call(
        functools.partial(fetch_kernel, parts, group),
        out_shape=pltpu.HBM((blocks, feats + 4, cap), BF16),
        in_specs=[WHOLE_VMEM, WHOLE_VMEM, IN_HBM, IN_HBM],
        out_specs=IN_HBM,
        scratch_shapes=[
            pltpu.VMEM((feats, left), BF16),
            pltpu.VMEM((n, 128), F32),
            [pltpu.VMEM((cap, 128), F32) for _ in range(8)],
            pltpu.SMEM((blocks, cap), I32),
            pltpu.VMEM((blocks, feats + 4, cap), BF16),
            pltpu.VMEM((blocks, 8, cap), F32),
            pltpu.SemaphoreType.DMA((parts + 3,)),
            pltpu.SemaphoreType.DMA((blocks // group,)),
        ],
        compiler_params=params(40),
        name="fetch",
    )(idx, head, pltpu.with_memory_space_constraint(extra, pltpu.HBM), pltpu.with_memory_space_constraint(table_t, pltpu.HBM))


PARTS = 6


def room_of(cap):
    return cap // PARTS


def lane_part(shape, cap):
    lane = lax.broadcasted_iota(I32, shape, len(shape) - 1)
    part = lane // room_of(cap)
    return jnp.where(part < PARTS, part, -1), lane % room_of(cap)


def ask_kernel(off, req2_ref, seeds_ref, extra_ref, rank_ref):
    blocks, cap = req2_ref.shape
    own = seeds_ref[0:1, :]
    seeds = own.shape[1]
    room = room_of(cap)
    owner, slot = own // cap, own % cap

    def bits(mask):
        return jnp.where(mask, 1.0, 0.0).astype(BF16)

    mine = bits(lax.broadcasted_iota(I32, (blocks, seeds), 0) == owner)
    before = bits(lax.broadcasted_iota(I32, (seeds, seeds), 0) < lax.broadcasted_iota(I32, (seeds, seeds), 1))
    mine32 = mine.astype(F32)
    rank = jnp.sum(mine32 * jnp.dot(mine, before, preferred_element_type=F32), axis=0, keepdims=True)
    rank_ref[...] = rank
    at_slot = bits(lax.broadcasted_iota(I32, (cap, seeds), 0) == slot)
    lane = lax.broadcasted_iota(I32, (cap, seeds), 0)
    entry = jnp.where(lane // room < PARTS, lane % room, -1).astype(F32)
    at_rank = bits(entry == rank)
    full = jnp.max(jnp.where(rank >= room, 1.0, 0.0))
    last = lax.broadcasted_iota(I32, (blocks, cap), 1) == cap - 1
    extra_ref[...] = jnp.zeros_like(extra_ref)
    for k, part in enumerate((req2_ref[...] // cap, req2_ref[...] % cap)):
        part = part.astype(F32)
        extra_ref[:, off + k, :] = part
        node = jnp.dot(part.astype(BF16), at_slot, preferred_element_type=F32) * mine32
        listed = lax.dot_general(node.astype(BF16), at_rank, (((1,), (1,)), ((), ())), preferred_element_type=F32)
        extra_ref[:, off + 2 + k, :] = jnp.where(last, full, listed)


def ask(req2_rows, seed_list, feats):
    blocks, cap = req2_rows.shape
    return pl.pallas_call(
        functools.partial(ask_kernel, feats % 8),
        out_shape=(
            pltpu.HBM((blocks, 8, cap), F32),
            jax.ShapeDtypeStruct((1, seed_list.shape[1]), F32),
        ),
        in_specs=[WHOLE_VMEM, WHOLE_VMEM],
        out_specs=(WHOLE_VMEM, WHOLE_VMEM),
        compiler_params=params(8),
        name="ask",
    )(req2_rows, seed_list)


def own_weight(fanout):
    return 1 << fanout.bit_length()


def codes_kernel(own, cap, count_ref, list_ref, out_ref):
    depth, width = list_ref.shape
    each = out_ref.shape[1] // cap
    zero = jnp.zeros((16, width), BF16)
    hit = [jnp.full((16, width), own if k == 0 else 1, BF16) for k in range(2)]

    def step(t, _):
        o = pl.program_id(1) * each + t
        local = list_ref[...] - o * cap
        live = (local >= 0) & (local < count_ref[o])
        local = jnp.where(live, local, -1).astype(F32)
        want = [jnp.broadcast_to(local[k : k + 1], (16, width)).astype(BF16) for k in range(depth)]
        for g in range(cap // 16):
            slot = (lax.broadcasted_iota(I32, (16, width), 0) + g * 16).astype(F32).astype(BF16)
            total = jnp.where(want[0] == slot, hit[0], zero)
            for k in range(1, depth):
                total = total + jnp.where(want[k] == slot, hit[1], zero)
            out_ref[0, pl.ds(pl.multiple_of(t * cap + g * 16, 16), 16), :] = total
        return 0

    lax.fori_loop(0, each, step, 0)


def codes(counts, lists, cap, place):
    depth, nodes = lists.shape
    blocks = counts.shape[0]
    width = 256
    each = 8
    return pl.pallas_call(
        functools.partial(codes_kernel, own_weight(depth - 1), cap),
        grid=(nodes // width, blocks // each),
        out_shape=place((nodes // width, blocks * cap, width), BF16),
        in_specs=[WHOLE_SMEM, pl.BlockSpec((depth, width), lambda q, o: (0, q))],
        out_specs=pl.BlockSpec((1, each * cap, width), lambda q, o: (q, o, 0)),
        compiler_params=params(8),
        name="codes",
    )(counts, lists)


def rank_codes_kernel(own, cap, count_ref, list_ref, rank_ref, out_ref):
    depth, width = list_ref.shape
    each = out_ref.shape[0] // cap
    zero = jnp.zeros((16, width), BF16)
    hit = [jnp.full((16, width), v, BF16) for v in (own, 1)]

    def step(t, _):
        o = pl.program_id(0) * each + t
        local = list_ref[...] - o * cap
        live = (local >= 0) & (local < count_ref[o])
        local = jnp.where(live, local, -1).astype(F32)
        rank = jnp.where(live[0:1], rank_ref[...], -cap * 1.0)
        rank = jnp.where(rank < room_of(cap), rank, -cap * 1.0)
        rows = [rank + q * room_of(cap) for q in range(PARTS)] + [local[k : k + 1] for k in range(1, depth)]
        want = [jnp.broadcast_to(row, (16, width)).astype(BF16) for row in rows]
        for g in range(cap // 16):
            slot = (lax.broadcasted_iota(I32, (16, width), 0) + g * 16).astype(F32).astype(BF16)
            total = jnp.where(want[0] == slot, hit[0], zero)
            for k in range(1, len(rows)):
                total = total + jnp.where(want[k] == slot, hit[k >= PARTS], zero)
            out_ref[pl.ds(pl.multiple_of(t * cap + g * 16, 16), 16), :] = total
        return 0

    lax.fori_loop(0, each, step, 0)


def rank_codes(counts, lists, rank, cap):
    depth, seeds = lists.shape
    blocks = counts.shape[0]
    each = 8
    return pl.pallas_call(
        functools.partial(rank_codes_kernel, own_weight(depth - 1), cap),
        grid=(blocks // each,),
        out_shape=jax.ShapeDtypeStruct((blocks * cap, seeds), BF16),
        in_specs=[WHOLE_SMEM, WHOLE_VMEM, WHOLE_VMEM],
        out_specs=pl.BlockSpec((each * cap, seeds), lambda o: (o, 0)),
        compiler_params=params(8),
        name="rank_codes",
    )(counts, lists, rank)


def split_codes(code, own):
    return jnp.where(code >= own, jnp.ones((), BF16), jnp.zeros((), BF16))


def layer_kernel(
    fanout, got_ref, first_ref, codes_hbm, ws_ref, wn_ref, b_ref, w2_ref, out_v, terms_ref, flag_ref, codes_v, got_v, choose_v, terms_v, sems
):
    blocks, _, cap = got_ref.shape
    feats = got_v.shape[0]
    rest, slots, width = codes_v.shape
    parts = rest + 1
    pairs, nodes = blocks // 2, choose_v.shape[1]
    half = w2_ref.shape[0] // 2
    deep = half // PARTS
    own_w = own_weight(fanout)
    def load(q):
        return pltpu.make_async_copy(codes_hbm.at[q], codes_v.at[q], sems.at[q])

    for q in range(rest):
        load(q).start()
    one, zero = jnp.ones((16, 2 * cap), BF16), jnp.zeros((16, 2 * cap), BF16)

    def fill(asked, p):
        for base in range(0, nodes, 256):
            local = asked - base
            local = jnp.where((local >= 0) & (local < 256), local, -1.0)
            want = jnp.broadcast_to(local, (16, 2 * cap)).astype(BF16)
            for g in range(0, 256, 16):
                node = (lax.broadcasted_iota(I32, (16, 2 * cap), 0) + g).astype(F32).astype(BF16)
                choose_v[p, base + g : base + g + 16, :] = jnp.where(want == node, one, zero)

    def asked_of(o, row):
        asked = got_ref[o, feats : feats + 4].astype(F32)
        return asked[row : row + 1] * cap + asked[row + 1 : row + 2]

    def choose(p, _):
        for u in range(2):
            o = 2 * p + u
            got_v[:, pl.ds(pl.multiple_of(o * cap, cap), cap)] = got_ref[o, :feats]
        fill(jnp.concatenate([asked_of(2 * p, 0), asked_of(2 * p + 1, 0)], axis=1), p)
        return 0

    lax.fori_loop(0, pairs, choose, 0)
    part, _ = lane_part((1, cap), cap)
    for p in range(pairs, choose_v.shape[0]):
        both = []
        for c in (2 * (p - pairs), 2 * (p - pairs) + 1):
            asked = jnp.full((1, cap), -1.0, F32)
            for u in range(max(0, min(PARTS, blocks - c * PARTS))):
                asked = jnp.where(part == u, asked_of(c * PARTS + u, 2), asked)
            both.append(asked)
        fill(jnp.concatenate(both, axis=1), p)
    flag = got_ref[0, feats + 2 : feats + 3].astype(F32)
    for o in range(1, blocks):
        flag = jnp.maximum(flag, got_ref[o, feats + 2 : feats + 3].astype(F32))
    flag_ref[...] = flag
    for q in range(parts):
        if q == 1:
            for k in range(rest):
                load(k).wait()
        code = codes_v[q - 1] if q else first_ref[0]
        both = jnp.dot(got_v[...], code, preferred_element_type=F32)
        own = jnp.dot(got_v[...], split_codes(code, own_w), preferred_element_type=F32)
        summed = ((both - own_w * own) / fanout).astype(BF16)
        pre = jnp.dot(ws_ref[...], own.astype(BF16), preferred_element_type=F32)
        pre = pre + jnp.dot(wn_ref[...], summed, preferred_element_type=F32) + b_ref[...]
        hidden = jnp.maximum(pre, 0.0).astype(BF16)
        terms = jnp.dot(w2_ref[...], hidden, preferred_element_type=F32)
        terms_v[:, q * width : (q + 1) * width] = terms.astype(BF16)

    terms_ref[...] = terms_v[:half]
    part8, _ = lane_part((deep, cap), cap)
    for p in range(pairs, choose_v.shape[0]):
        found = jnp.dot(terms_v[:half], choose_v[p], preferred_element_type=F32)
        for v in range(2):
            c = 2 * (p - pairs) + v
            for u in range(max(0, min(PARTS, blocks - c * PARTS))):
                block = jnp.zeros((deep, cap), F32)
                for q in range(PARTS):
                    piece = found[q * deep : (q + 1) * deep, v * cap : (v + 1) * cap]
                    piece = pltpu.roll(piece, (q - u) * room_of(cap) % cap, 1)
                    block = jnp.where(part8 == q, piece, block)
                out_v[c * PARTS + u, half:] = block.astype(BF16)
    for p in range(pairs):
        near = jnp.dot(terms_v[half:], choose_v[p], preferred_element_type=F32).astype(BF16)
        out_v[2 * p, :half] = near[:, :cap]
        out_v[2 * p + 1, :half] = near[:, cap:]


def layer(got, first, code, w1_self, w1_neigh, bias1, w2, fanout):
    blocks, _, cap = got.shape
    rest, slots, width = code.shape
    nodes = (rest + 1) * width
    half = w2.shape[0] // 2
    return pl.pallas_call(
        functools.partial(layer_kernel, fanout),
        out_shape=(
            pltpu.HBM((blocks, half + half // PARTS, cap), BF16),
            pltpu.HBM((half, nodes), BF16),
            jax.ShapeDtypeStruct((1, cap), F32),
        ),
        in_specs=[WHOLE_VMEM, WHOLE_VMEM, IN_HBM] + [WHOLE_VMEM] * 4,
        out_specs=(WHOLE_VMEM,) * 3,
        scratch_shapes=[
            pltpu.VMEM(code.shape, BF16),
            pltpu.VMEM((w1_self.shape[1], slots), BF16),
            pltpu.VMEM((blocks // 2 + -(-blocks // (2 * PARTS)), nodes, 2 * cap), BF16),
            pltpu.VMEM((w2.shape[0], nodes), BF16),
            pltpu.SemaphoreType.DMA((rest,)),
        ],
        compiler_params=params(40),
        name="layer",
    )(got, first, pltpu.with_memory_space_constraint(code, pltpu.HBM), w1_self, w1_neigh, bias1[:, None], w2)


def wide(ref, first, last, lo, hi):
    return jnp.concatenate([ref[o, lo:hi] for o in range(first, last)], axis=1)


def logits_kernel(fanout, got_ref, code_ref, b_ref, out_ref):
    blocks, half = got_ref.shape[0], got_ref.shape[1] // 2
    classes = out_ref.shape[0]
    own_w = own_weight(fanout)
    code = code_ref[0]
    own = split_codes(code, own_w)
    mine = jnp.dot(wide(got_ref, 0, blocks, 0, half), own, preferred_element_type=F32)
    near = jnp.dot(wide(got_ref, 0, blocks, half, 2 * half), code - own_w * own, preferred_element_type=F32) / fanout
    out_ref[...] = (mine + near)[:classes] + b_ref[...]


def final(got, code, bias2, fanout):
    return pl.pallas_call(
        functools.partial(logits_kernel, fanout),
        out_shape=jax.ShapeDtypeStruct((bias2.shape[0], code.shape[2]), F32),
        in_specs=[WHOLE_VMEM] * 3,
        out_specs=WHOLE_VMEM,
        compiler_params=params(20),
        name="logits",
    )(got, code, bias2[:, None])


def mask_rows(received, counts, capacity):
    is_live = (jnp.arange(capacity, dtype=jnp.int32)[None, :] < counts[:, None]).reshape(-1)
    flat = received.reshape(-1, received.shape[-1])
    return jnp.where(is_live[:, None], flat, jnp.zeros((), flat.dtype))


def right_product(rows, weight):
    return lax.dot_general(
        rows, weight, (((1,), (1,)), ((), ())), preferred_element_type=jnp.float32
    )


def plain_body(
    table_t,
    req_rows,
    count1,
    frontier_list,
    req2_rows,
    count2,
    seed_list,
    w1_self,
    w1_neigh,
    bias1,
    w2_self,
    w2_neigh,
    bias2,
):
    feat_width = table_t.shape[0]
    capacity = req_rows.shape[1]
    table_rows = table_t.T
    picked_rows = jnp.take(
        table_rows,
        lax.all_to_all(req_rows, AXES, split_axis=0, concat_axis=0, tiled=True),
        axis=0,
    )
    received = lax.all_to_all(
        picked_rows, AXES, split_axis=0, concat_axis=0, tiled=True
    )
    flat = mask_rows(received, count1, capacity)
    fanout_two = frontier_list.shape[0] - 1
    front_nodes = frontier_list.shape[1]
    picked = jnp.take(flat, frontier_list.reshape(-1), axis=0).reshape(
        fanout_two + 1, front_nodes, feat_width
    )
    summed = (jnp.sum(picked[1:].astype(jnp.float32), axis=0) / fanout_two).astype(jnp.bfloat16)
    preact = right_product(picked[0], w1_self) + right_product(summed, w1_neigh) + bias1[None, :]
    hidden_rows = jax.nn.relu(preact).astype(jnp.bfloat16)
    cap_two = req2_rows.shape[1]
    payload = jnp.concatenate(
        [right_product(hidden_rows, w2_self), right_product(hidden_rows, w2_neigh)], axis=1
    )
    chosen = jnp.take(
        payload,
        lax.all_to_all(req2_rows, AXES, split_axis=0, concat_axis=0, tiled=True),
        axis=0,
    )
    got_back = lax.all_to_all(chosen, AXES, split_axis=0, concat_axis=0, tiled=True)
    flat_two = mask_rows(got_back, count2, cap_two)
    fanout_one = seed_list.shape[0] - 1
    seed_nodes = seed_list.shape[1]
    picked_two = jnp.take(flat_two, seed_list.reshape(-1), axis=0).reshape(
        fanout_one + 1, seed_nodes, flat_two.shape[1]
    )
    classes = w2_self.shape[0]
    near = jnp.sum(picked_two[1:, :, classes:], axis=0) / fanout_one
    logits = (picked_two[0, :, :classes] + near).T + bias2[:, None]
    return logits


def rank_logits_kernel(fanout, got_ref, code_ref, b_ref, out_ref):
    blocks, rows, cap = got_ref.shape
    deep = rows // (PARTS + 1)
    half = rows - deep
    own_w = own_weight(fanout)
    code = code_ref[...]
    own = split_codes(code, own_w)
    part, _ = lane_part((deep, cap), cap)

    def spread(o):
        terms = got_ref[o, half:].astype(F32)
        return jnp.concatenate([jnp.where(part == q, terms, 0.0) for q in range(PARTS)], axis=0).astype(BF16)

    mine = jnp.dot(jnp.concatenate([spread(o) for o in range(blocks)], axis=1), own, preferred_element_type=F32)
    near = jnp.dot(wide(got_ref, 0, blocks, 0, half), code - own_w * own, preferred_element_type=F32) / fanout
    out_ref[...] = (mine + near)[: out_ref.shape[0]] + b_ref[...]


def rank_final(got, code, bias2, fanout):
    return pl.pallas_call(
        functools.partial(rank_logits_kernel, fanout),
        out_shape=pltpu.HBM((bias2.shape[0], code.shape[1]), F32),
        in_specs=[WHOLE_VMEM] * 3,
        out_specs=WHOLE_VMEM,
        compiler_params=params(20),
        name="rank_logits",
    )(got, code, bias2[:, None])


HEAD = 6656
MOST = 8 << 20


def body(
    table_t,
    req_rows,
    count1,
    frontier_list,
    req2_rows,
    count2,
    seed_list,
    w1_self,
    w1_neigh,
    bias1,
    w2_self,
    w2_neigh,
    bias2,
):
    cap = req_rows.shape[1]
    fits = req_rows.size * frontier_list.shape[1] <= MOST and req2_rows.shape[1] == cap and table_t.shape[0] % 8 == 4
    fits = fits and table_t.shape[1] % 128 == 0 and table_t.shape[1] > HEAD
    if not fits or table_t.shape[1] > 32768 or frontier_list.shape[1] > 65536:
        return plain_body(
            table_t,
            req_rows,
            count1,
            frontier_list,
            req2_rows,
            count2,
            seed_list,
            w1_self,
            w1_neigh,
            bias1,
            w2_self,
            w2_neigh,
            bias2,
        )
    feats, fanout_two, fanout_one = table_t.shape[0], frontier_list.shape[0] - 1, seed_list.shape[0] - 1
    extra, rank = ask(req2_rows, seed_list, feats)
    got1 = exchange(fetch(exchange(req_rows), extra, table_t, head_rows(table_t, HEAD)))
    first = codes(count1, frontier_list[:, :256], cap, jax.ShapeDtypeStruct)
    code1 = codes(count1, frontier_list[:, 256:], cap, pltpu.HBM)
    classes = w2_self.shape[0]
    half = -(-classes // 48) * 48
    pad = ((0, half - classes), (0, 0))
    w2 = jnp.concatenate([jnp.pad(w2_self, pad), jnp.pad(w2_neigh, pad)], axis=0)
    out2, terms, flag = layer(got1, first, code1, w1_self, w1_neigh, bias1, w2, fanout_two)
    got2 = exchange(out2)
    logits = rank_final(got2, rank_codes(count2, seed_list, rank, cap), bias2, fanout_one)

    def in_full(logits):
        asked = exchange(req2_rows)
        own = jnp.take(terms, asked.reshape(-1), axis=1, mode="clip").reshape(half, -1, cap).transpose(1, 0, 2)
        got = jnp.concatenate([exchange(own), got2[:, :half]], axis=1)
        return final(got, codes(count2, seed_list, cap, jax.ShapeDtypeStruct), bias2, fanout_one)

    return lax.cond(flag[0, cap - 1] > 0.5, in_full, lambda logits: logits, logits)


def solution(mesh):
    split, split1 = P(AXES, None), P(AXES)
    cols = P(None, AXES)
    in_specs = (cols, split, split1, cols, split, split1, cols, P(), P(), P(), P(), P(), P())
    return jax.shard_map(body, mesh=mesh, in_specs=in_specs, out_specs=cols, check_vma=False)
```
